32 devices in a mesh: ctx: 4 (over x, core), fsdp: 8 (over z, y).
Axes of the slice: x: 2, y: 2, z: 4, core: 2. Of those that a mesh axis runs over, the one named last changes fastest.
Arguments:
- hidden_in: bfloat16 [8, 512, 1536], P('fsdp', 'ctx'), may hold values from -6 to 6
- segments: int32 [8, 512], P('fsdp', 'ctx'), may hold values from 0 to 3, never falling along the last dimension, each value on 1 to 384 neighbouring positions
- w_query: bfloat16 [1536, 1536], P('fsdp'), may hold values from -0.15625 to 0.15625
- w_key: bfloat16 [1536, 768], P('fsdp'), may hold values from -0.15625 to 0.15625
- w_value: bfloat16 [1536, 768], P('fsdp'), may hold values from -0.15625 to 0.15625
- w_out: bfloat16 [1536, 1536], P('fsdp'), may hold values from -0.875 to 0.875
- w_gate: bfloat16 [1536, 4096], P('fsdp'), may hold values from -0.15625 to 0.15625
- w_up: bfloat16 [1536, 4096], P('fsdp'), may hold values from -0.15625 to 0.15625
- w_down: bfloat16 [4096, 1536], P('fsdp'), may hold values from -0.09375 to 0.09375
- attn_gain: bfloat16 [1536], P('fsdp'), may hold values from 0.5 to 1.5
- ffn_gain: bfloat16 [1536], P('fsdp'), may hold values from 0.5 to 1.5
- grad_out: bfloat16 [8, 512, 1536], P('fsdp', 'ctx'), may hold values from -6 to 6
Outputs:
- output: bfloat16 [8, 512, 1536], P('fsdp', 'ctx')
- grad_in: float32 [8, 512, 1536], P('fsdp', 'ctx')
- grad_w_query: float32 [1536, 1536], P(('ctx', 'fsdp'))
- grad_w_key: float32 [1536, 768], P(('ctx', 'fsdp'))
- grad_w_value: float32 [1536, 768], P(('ctx', 'fsdp'))
- grad_w_out: float32 [1536, 1536], P(('ctx', 'fsdp'))
- grad_w_gate: float32 [1536, 4096], P(('ctx', 'fsdp'))
- grad_w_up: float32 [1536, 4096], P(('ctx', 'fsdp'))
- grad_w_down: float32 [4096, 1536], P(('ctx', 'fsdp'))
- grad_attn_gain: float32 [1536], P(('ctx', 'fsdp'))
- grad_ffn_gain: float32 [1536], P(('ctx', 'fsdp'))
The draws below stay inside these ranges and needn't reach their ends.
Inputs may be any that keep to these rules, and one draw needn't show every extreme that they name: `segments`: segment numbers never fall along a sequence.
All inputs are finite; a program needn't handle non-finite values.
Results may differ from the reference program's by a relative error of at most 0.014.
Values may be sent and summed in bfloat16 or wider, within the bound.
A program may use at most 192 MiB of HBM per device.

```python
import math
import jax
import jax.numpy as jnp
import numpy as np
from jax import lax

D = 1536
HEADS = 16
KV_HEADS = 8
HEAD_DIM = 96
FF = 4096
SEQ_LEN = 512
SEQS = 8


def level_of(own_key, dims, split, smallest, largest):
    level, own = 1.0, jax.random.fold_in(own_key, 6)
    for position, parts in split:
        heights = jnp.exp(jax.random.uniform(jax.random.fold_in(own, position), (parts,), jnp.float32, smallest / len(split), largest / len(split)))
        level = level * jnp.repeat(heights, dims[position] // parts).reshape([-1 if axis == position else 1 for axis in range(len(dims))])
    return level


def length_profile(number_of, total, limit, slope):
    weights = [(1 << 20) // math.isqrt(standing ** slope) + 1 for standing in range(2, number_of + 1)]
    surplus, given = total - limit - (number_of - 1), [1] * (number_of - 1)
    while surplus > 0:
        free = [i for i in range(number_of - 1) if given[i] < limit]
        pool, left = sum([weights[i] for i in free]), surplus
        for i in free:
            more = min(limit - given[i], max(1, left * weights[i] // pool), surplus)
            given[i] = given[i] + more
            surplus = surplus - more
    return np.array([limit] + given)


def uneven_parts(key, count, total, limit, skew):
    if count == 2:
        one = jax.random.randint(key, (), max(1, total - limit), min(limit, total - 1) + 1)
        return jnp.stack([one, total - one])
    sizes = jnp.asarray(length_profile(count, total, limit, skew), jnp.int32)
    pairs = (count - 1) // 2
    source_of, sink = sizes[1:1 + 2 * pairs:2], sizes[2:2 + 2 * pairs:2]
    slack = jnp.minimum(source_of - 1, limit - sink)
    moved = jax.random.randint(jax.random.fold_in(key, 1), (pairs,), 0, 1 << 20) % (slack + 1)
    sizes = sizes.at[1:1 + 2 * pairs:2].set(source_of - moved).at[2:2 + 2 * pairs:2].set(sink + moved)
    return sizes[jax.random.permutation(jax.random.fold_in(key, 2), count)]


def gaussian(stream_key, extent, deviation, bound, cuts=(), kind=jnp.bfloat16):
    entries = jax.random.normal(stream_key, extent, jnp.float32) * deviation
    if len(cuts) > 0:
        entries = level_of(stream_key, extent, cuts, -0.22, 0.18) * entries
    return jnp.clip(entries, min=-bound, max=bound).astype(kind)


def setup_inputs(seed: int = 0) -> dict:
    arg_keys = jax.random.split(jax.random.key(seed), 13)
    hidden_in = gaussian(arg_keys[0], (SEQS, SEQ_LEN, D), 1.0, 6.0, ((0, 8), (1, 4)))
    segments = jax.vmap(lambda own: jnp.searchsorted(jnp.cumsum(uneven_parts(own, 4, SEQ_LEN, SEQ_LEN * 3 // 4, 0)), jnp.arange(SEQ_LEN), side="right"))(jax.random.split(arg_keys[1], SEQS)).reshape((SEQS, SEQ_LEN)).astype(jnp.int32)
    w_query = gaussian(arg_keys[2], (D, HEADS * HEAD_DIM), D ** -0.5, 0.15625, ((0, 8),))
    w_key = gaussian(arg_keys[3], (D, KV_HEADS * HEAD_DIM), D ** -0.5, 0.15625, ((0, 8),))
    w_value = gaussian(arg_keys[4], (D, KV_HEADS * HEAD_DIM), D ** -0.5, 0.15625, ((0, 8),))
    w_out = gaussian(arg_keys[5], (HEADS * HEAD_DIM, D), (HEADS * HEAD_DIM // 32) ** -0.5, 0.875, ((0, 8),))
    w_gate = gaussian(arg_keys[6], (D, FF), D ** -0.5, 0.15625, ((0, 8),))
    w_up = gaussian(arg_keys[7], (D, FF), D ** -0.5, 0.15625, ((0, 8),))
    w_down = gaussian(arg_keys[8], (FF, D), FF ** -0.5, 0.09375, ((0, 8),))
    attn_gain = jnp.clip(1.0 + 0.1 * jax.random.normal(arg_keys[9], (D,), jnp.float32), 0.5, 1.5).astype(jnp.bfloat16)
    ffn_gain = jnp.clip(1.0 + 0.1 * jax.random.normal(arg_keys[10], (D,), jnp.float32), 0.5, 1.5).astype(jnp.bfloat16)
    grad_out = gaussian(arg_keys[11], (SEQS, SEQ_LEN, D), 1.0, 6.0, ((0, 8), (1, 4)))
    return dict(hidden_in=hidden_in, segments=segments, w_query=w_query, w_key=w_key, w_value=w_value, w_out=w_out, w_gate=w_gate, w_up=w_up, w_down=w_down, attn_gain=attn_gain, ffn_gain=ffn_gain, grad_out=grad_out)


EPS = 1e-05
ROPE_BASE = 100000.0

def norm_forward(values_in, norm_gain):
    inv_rms = lax.rsqrt(lax.optimization_barrier(jnp.mean(values_in * values_in, axis=-1, keepdims=True)) + EPS)
    scaled = values_in * inv_rms
    normed = (scaled * norm_gain.astype(jnp.float32)).astype(jnp.bfloat16)
    return (normed, scaled, inv_rms)

def norm_backward(grad_normed, scaled, inv_rms, norm_gain):
    grad_scaled = grad_normed * norm_gain.astype(jnp.float32)
    grad_gain = lax.optimization_barrier(jnp.sum(grad_normed * scaled, axis=0))
    grad_input = inv_rms * (grad_scaled - scaled * lax.optimization_barrier(jnp.mean(grad_scaled * scaled, axis=-1, keepdims=True)))
    return (grad_input, grad_gain)

def rope_tables(positions):
    half_dim = HEAD_DIM // 2
    freq_index = jnp.arange(half_dim, dtype=jnp.float32)
    frequency = jnp.exp(freq_index * (-2.0 / HEAD_DIM) * math.log(ROPE_BASE))
    angles = positions.astype(jnp.float32)[:, :, None] * frequency
    return (jnp.cos(angles)[:, :, None, :], jnp.sin(angles)[:, :, None, :])

def rotate(tensor, cosine_table, sine_table):
    half_dim = tensor.shape[-1] // 2
    front_half = tensor[..., :half_dim]
    back_half = tensor[..., half_dim:]
    return jnp.concatenate([front_half * cosine_table - back_half * sine_table, back_half * cosine_table + front_half * sine_table], axis=-1)

def rotate_back(tensor, cosine_table, sine_table):
    half_dim = tensor.shape[-1] // 2
    front_half = tensor[..., :half_dim]
    back_half = tensor[..., half_dim:]
    return jnp.concatenate([front_half * cosine_table + back_half * sine_table, back_half * cosine_table - front_half * sine_table], axis=-1)

def layout(seg_query, seg_keys, run_start):
    run_len = seg_query.shape[1]
    key_len = seg_keys.shape[1]
    row_ids = run_start + jnp.arange(run_len, dtype=jnp.int32)
    col_ids = jnp.arange(key_len, dtype=jnp.int32)
    before = lax.optimization_barrier(jnp.sum((seg_keys[:, None, :] < seg_query[:, :, None]).astype(jnp.int32), axis=-1))
    positions = row_ids[None, :] - before
    allowed = (seg_keys[:, None, :] == seg_query[:, :, None]) & (col_ids[None, None, :] <= row_ids[None, :, None])
    return (positions, allowed)

def masked_scores(queries, key_rows, allowed):
    seq_count, run_len, head_count, head_dim = queries.shape
    kv_count = key_rows.shape[2]
    grouped = queries.reshape(seq_count, run_len, kv_count, head_count // kv_count, head_dim)
    raw_scores = jnp.einsum('brkgd,bskd->bkgrs', grouped.astype(jnp.float32), key_rows.astype(jnp.float32)) * head_dim ** (-0.5)
    return (grouped, jnp.where(allowed[:, None, None], raw_scores, -1e+30))

def attend(queries, key_rows, value_rows, allowed):
    grouped, scores = masked_scores(queries, key_rows, allowed)
    row_max = lax.optimization_barrier(jnp.max(scores, axis=-1, keepdims=True))
    row_sum = lax.optimization_barrier(jnp.sum(jnp.exp(scores - row_max), axis=-1, keepdims=True))
    log_total = row_max + jnp.log(row_sum)
    prob_low = jnp.exp(scores - log_total).astype(jnp.bfloat16)
    mixed_rows = jnp.einsum('bkgrs,bskd->brkgd', prob_low.astype(jnp.float32), value_rows.astype(jnp.float32))
    return (mixed_rows.reshape(queries.shape).astype(jnp.bfloat16), log_total)

def attend_back(queries, key_rows, value_rows, allowed, log_total, out_rows, cotangent):
    grouped, scores = masked_scores(queries, key_rows, allowed)
    seq_count, run_len, kv_count, group_size, head_dim = grouped.shape
    probs = jnp.exp(scores - log_total)
    prob_low = probs.astype(jnp.bfloat16)
    grad_grouped = cotangent.reshape(grouped.shape).astype(jnp.float32)
    grad_probs = jnp.einsum('brkgd,bskd->bkgrs', grad_grouped, value_rows.astype(jnp.float32))
    row_delta = lax.optimization_barrier(jnp.sum(cotangent.astype(jnp.float32) * out_rows.astype(jnp.float32), axis=-1))
    row_delta = jnp.transpose(row_delta.reshape(seq_count, run_len, kv_count, group_size), (0, 2, 3, 1))[..., None]
    grad_scores = (probs * (grad_probs - row_delta)).astype(jnp.bfloat16).astype(jnp.float32)
    score_scale = head_dim ** (-0.5)
    grad_query = jnp.einsum('bkgrs,bskd->brkgd', grad_scores, key_rows.astype(jnp.float32)) * score_scale
    grad_key = jnp.einsum('bkgrs,brkgd->bskd', grad_scores, grouped.astype(jnp.float32)) * score_scale
    grad_value = jnp.einsum('bkgrs,brkgd->bskd', prob_low.astype(jnp.float32), grad_grouped)
    return (grad_query.reshape(queries.shape), grad_key, grad_value)

def one_sequence(hidden_seq, seg_seq, cotangent_seq, params):
    w_query, w_key, w_value, w_out, w_gate, w_up, w_down, attn_gain, ffn_gain = params
    seg_rows = seg_seq[None]
    positions, allowed = layout(seg_rows, seg_rows, 0)
    cosine_table, sine_table = rope_tables(positions)
    flat_in = hidden_seq.astype(jnp.float32)
    attn_normed, attn_scaled, attn_recip = norm_forward(flat_in, attn_gain)
    query_proj = jnp.dot(attn_normed, w_query, preferred_element_type=jnp.float32).reshape(1, SEQ_LEN, HEADS, HEAD_DIM)
    key_proj = jnp.dot(attn_normed, w_key, preferred_element_type=jnp.float32).reshape(1, SEQ_LEN, KV_HEADS, HEAD_DIM)
    value_proj = jnp.dot(attn_normed, w_value, preferred_element_type=jnp.float32).reshape(1, SEQ_LEN, KV_HEADS, HEAD_DIM)
    rot_query = rotate(query_proj, cosine_table, sine_table).astype(jnp.bfloat16)
    rot_key = rotate(key_proj, cosine_table, sine_table).astype(jnp.bfloat16)
    value_low = value_proj.astype(jnp.bfloat16)
    attn_rows, log_total = attend(rot_query, rot_key, value_low, allowed)
    attn_flat = attn_rows.reshape(SEQ_LEN, HEADS * HEAD_DIM)
    mid_stream = flat_in + jnp.dot(attn_flat, w_out, preferred_element_type=jnp.float32)
    ffn_normed, ffn_scaled, ffn_recip = norm_forward(mid_stream, ffn_gain)
    gate_proj = jnp.dot(ffn_normed, w_gate, preferred_element_type=jnp.float32)
    up_proj = jnp.dot(ffn_normed, w_up, preferred_element_type=jnp.float32)
    sigmoid_gate = jax.nn.sigmoid(gate_proj)
    silu_gate = gate_proj * sigmoid_gate
    inner_act = (silu_gate * up_proj).astype(jnp.bfloat16)
    output = (mid_stream + jnp.dot(inner_act, w_down, preferred_element_type=jnp.float32)).astype(jnp.bfloat16)
    grad_low = cotangent_seq
    grad_w_down = jnp.dot(inner_act.T, grad_low, preferred_element_type=jnp.float32)
    grad_inner = jnp.dot(grad_low, w_down.T, preferred_element_type=jnp.float32)
    grad_gate = (grad_inner * up_proj * sigmoid_gate * (1.0 + gate_proj * (1.0 - sigmoid_gate))).astype(jnp.bfloat16)
    grad_up = (grad_inner * silu_gate).astype(jnp.bfloat16)
    grad_w_gate = jnp.dot(ffn_normed.T, grad_gate, preferred_element_type=jnp.float32)
    grad_w_up = jnp.dot(ffn_normed.T, grad_up, preferred_element_type=jnp.float32)
    grad_ffn_normed = jnp.dot(grad_gate, w_gate.T, preferred_element_type=jnp.float32) + jnp.dot(grad_up, w_up.T, preferred_element_type=jnp.float32)
    grad_mid_norm, grad_ffn_gain = norm_backward(grad_ffn_normed, ffn_scaled, ffn_recip, ffn_gain)
    grad_mid = grad_low.astype(jnp.float32) + grad_mid_norm
    grad_mid_low = grad_mid.astype(jnp.bfloat16)
    grad_w_out = jnp.dot(attn_flat.T, grad_mid_low, preferred_element_type=jnp.float32)
    grad_attn = jnp.dot(grad_mid_low, w_out.T, preferred_element_type=jnp.float32).astype(jnp.bfloat16)
    grad_attn = grad_attn.reshape(1, SEQ_LEN, HEADS, HEAD_DIM)
    grad_rq, grad_rk, grad_value = attend_back(rot_query, rot_key, value_low, allowed, log_total, attn_rows, grad_attn)
    grad_query_low = rotate_back(grad_rq, cosine_table, sine_table).astype(jnp.bfloat16).reshape(SEQ_LEN, HEADS * HEAD_DIM)
    grad_key_low = rotate_back(grad_rk, cosine_table, sine_table).astype(jnp.bfloat16).reshape(SEQ_LEN, KV_HEADS * HEAD_DIM)
    grad_value_low = grad_value.astype(jnp.bfloat16).reshape(SEQ_LEN, KV_HEADS * HEAD_DIM)
    grad_w_query = jnp.dot(attn_normed.T, grad_query_low, preferred_element_type=jnp.float32)
    grad_w_key = jnp.dot(attn_normed.T, grad_key_low, preferred_element_type=jnp.float32)
    grad_w_value = jnp.dot(attn_normed.T, grad_value_low, preferred_element_type=jnp.float32)
    grad_attn_normed = jnp.dot(grad_query_low, w_query.T, preferred_element_type=jnp.float32) + jnp.dot(grad_key_low, w_key.T, preferred_element_type=jnp.float32) + jnp.dot(grad_value_low, w_value.T, preferred_element_type=jnp.float32)
    grad_in_norm, grad_attn_gain = norm_backward(grad_attn_normed, attn_scaled, attn_recip, attn_gain)
    grad_in = grad_mid + grad_in_norm
    weight_grads = (grad_w_query, grad_w_key, grad_w_value, grad_w_out, grad_w_gate, grad_w_up, grad_w_down, grad_attn_gain, grad_ffn_gain)
    return (output, grad_in, weight_grads)

def reference(hidden_in, segments, w_query, w_key, w_value, w_out, w_gate, w_up, w_down, attn_gain, ffn_gain, grad_out):
    params = (w_query, w_key, w_value, w_out, w_gate, w_up, w_down, attn_gain, ffn_gain)
    zeros_init = tuple((jnp.zeros(weight.shape, jnp.float32) for weight in params))

    def scan_step(running, per_sequence):
        hidden_seq, seg_seq, cotangent_seq = per_sequence
        output, grad_in, weight_grads = one_sequence(hidden_seq, seg_seq, cotangent_seq, params)
        return (tuple((total + part for total, part in zip(running, weight_grads))), (output, grad_in))
    running, (outputs, grad_inputs) = lax.scan(scan_step, zeros_init, (hidden_in, segments, grad_out))
    return (outputs, grad_inputs, running[0], running[1], running[2], running[3], running[4], running[5], running[6], running[7], running[8])
```

```python
import math

import jax
import jax.numpy as jnp
from jax import lax
from jax.sharding import PartitionSpec as P

HEADS = 16
KV_HEADS = 8
HEAD_DIM = 96
EPS = 1e-05
ROPE_BASE = 100000.0


def inverse_rms(values):
    return lax.rsqrt(jnp.mean(values * values, axis=-1, keepdims=True) + EPS)


def norm_backward(grad_normed, scaled, inv_rms, gain):
    grad_scaled = grad_normed * gain
    return inv_rms * (
        grad_scaled - scaled * jnp.mean(grad_scaled * scaled, axis=-1, keepdims=True)
    )


def rope_tables(positions):
    half_dim = HEAD_DIM // 2
    freq_index = jnp.arange(half_dim, dtype=jnp.float32)
    frequency = jnp.exp(freq_index * (-2.0 / HEAD_DIM) * math.log(ROPE_BASE))
    angles = positions.astype(jnp.float32)[:, None] * frequency
    return (jnp.cos(angles)[:, None, :], jnp.sin(angles)[:, None, :])


def rotate(tensor, cosine, sine):
    half_dim = tensor.shape[-1] // 2
    front, back = tensor[..., :half_dim], tensor[..., half_dim:]
    return jnp.concatenate([front * cosine - back * sine, back * cosine + front * sine], axis=-1)


def rotate_back(tensor, cosine, sine):
    return rotate(tensor, cosine, -sine)


def dot(left, right):
    return jnp.dot(left, right, preferred_element_type=jnp.float32)


def contract_rows(left, right):
    return lax.dot_general(
        left, right, (((0,), (0,)), ((), ())), preferred_element_type=jnp.float32
    )


def times_transpose(left, weight):
    return lax.dot_general(
        left, weight, (((1,), (1,)), ((), ())), preferred_element_type=jnp.float32
    )


def make_step(ctx_size, fsdp_size):
    depth = fsdp_size // 2
    low = jnp.bfloat16

    core_pairs = [(c, c ^ 1) for c in range(ctx_size)]
    x_pairs = [(c, c ^ 2) for c in range(ctx_size)]
    y_pairs = [(f, f ^ 1) for f in range(fsdp_size)]

    def z_pairs(shift):
        return [(f, (f // 2 + shift) % depth * 2 + f % 2) for f in range(fsdp_size)]

    owner_pairs = [
        (c * fsdp_size + f, ctx_size * f + c) for c in range(ctx_size) for f in range(fsdp_size)
    ]

    def to_core(value):
        return lax.ppermute(value, "ctx", core_pairs)

    def to_x(value):
        return lax.ppermute(value, "ctx", x_pairs)

    def to_y(value):
        return lax.ppermute(value, "fsdp", y_pairs)

    def to_z(value, shift):
        return lax.ppermute(value, "fsdp", z_pairs(shift))

    def gather_runs(own):
        pair = jnp.concatenate([own, to_x(own)], axis=0)
        return jnp.concatenate([pair, to_core(pair)], axis=0)

    def gather_pair(pair):
        return jnp.concatenate([pair, to_core(pair)], axis=0)

    def reduce_core(partial):
        half = partial.shape[0] // 2
        received = to_core(partial[half:].astype(low))
        return partial[:half] + received.astype(jnp.float32)

    def reduce_pair(partial):
        pair = reduce_core(partial).astype(low)
        other = to_x(pair)
        half = pair.shape[0] // 2
        other = jnp.concatenate([other[half:], other[:half]], axis=0)
        return pair.astype(jnp.float32) + other.astype(jnp.float32)

    def reduce_own(partial):
        pair = reduce_core(partial)
        half = pair.shape[0] // 2
        return pair[:half] + to_x(pair[half:].astype(low)).astype(jnp.float32)

    def gather_rows(block):
        f_index = lax.axis_index("fsdp")
        row, column = f_index // 2, f_index % 2
        arrived = [block] + [to_z(block, shift) for shift in range(1, depth)]
        beside = [to_y(one) for one in arrived]
        stacked = jnp.zeros((fsdp_size, *block.shape), block.dtype)
        for shift in range(depth):
            source = (row + depth - shift) % depth * 2
            tail = (0,) * block.ndim
            stacked = lax.dynamic_update_slice(
                stacked, arrived[shift][None], (source + column, *tail)
            )
            stacked = lax.dynamic_update_slice(
                stacked, beside[shift][None], (source + 1 - column, *tail)
            )
        return stacked

    def scatter_rows(parts, axis, wire=low):
        f_index = lax.axis_index("fsdp")
        row, column = f_index // 2, f_index % 2
        total = None
        for shift in [*range(1, depth), 0]:
            target = (row + shift) % depth * 2
            given = lax.dynamic_index_in_dim(parts, target + 1 - column, axis, keepdims=False)
            kept = lax.dynamic_index_in_dim(parts, target + column, axis, keepdims=False)
            summed = kept.astype(jnp.float32) + to_y(given).astype(jnp.float32)
            if shift:
                summed = to_z(summed.astype(wire), shift).astype(jnp.float32)
            total = summed if total is None else total + summed
        return total

    def spread_columns(blocks):
        c_index = lax.axis_index("ctx")
        count, rows, columns = blocks.shape
        result = jnp.zeros((rows, count, columns), jnp.float32)
        for bits, pairs in ((0, None), (1, core_pairs), (2, x_pairs), (3, None)):
            block = lax.dynamic_index_in_dim(blocks, c_index ^ bits, 0, keepdims=False)
            if bits:
                pairs = [(c, c ^ bits) for c in range(ctx_size)]
                block = lax.ppermute(block.astype(low), "ctx", pairs)
            result = lax.dynamic_update_slice(
                result, block.astype(jnp.float32)[:, None], (0, c_index ^ bits, 0)
            )
        return result

    def per_device(
        hidden_in,
        segments,
        w_query,
        w_key,
        w_value,
        w_out,
        w_gate,
        w_up,
        w_down,
        attn_gain,
        ffn_gain,
        grad_out,
    ):
        _, run_len, width = hidden_in.shape
        c_index = lax.axis_index("ctx")
        heads, kv_heads = HEADS // ctx_size, KV_HEADS // ctx_size
        q_cols, kv_cols = heads * HEAD_DIM, kv_heads * HEAD_DIM
        ff = w_gate.shape[1] // ctx_size
        shard = width // fsdp_size
        owned = shard // ctx_size

        def columns(weight, size):
            return lax.dynamic_slice_in_dim(weight, c_index * size, size, 1)

        def quarter(weight):
            rows = weight.shape[0] // ctx_size
            part = lax.dynamic_slice_in_dim(weight, c_index * rows, rows, 0)
            return lax.ppermute(part, ("ctx", "fsdp"), owner_pairs)

        seg_rows = gather_runs(segments.reshape(run_len, 1).astype(low).T)
        hidden = gather_runs(hidden_in.reshape(run_len, width))
        gains = gather_rows(jnp.stack([attn_gain, ffn_gain]))
        gains = jnp.swapaxes(gains, 0, 1).reshape(2, width).astype(jnp.float32)
        full_qkv = gather_rows(
            jnp.concatenate(
                [columns(w_query, q_cols), columns(w_key, kv_cols), columns(w_value, kv_cols)],
                axis=1,
            )
        ).reshape(width, q_cols + 2 * kv_cols)
        full_out = gather_rows(quarter(w_out)).reshape(q_cols, width)
        full_gate_up = gather_rows(
            jnp.concatenate([columns(w_gate, ff), columns(w_up, ff)], axis=1)
        ).reshape(width, 2 * ff)
        full_down = gather_rows(quarter(w_down)).reshape(ff, width)
        cotangent = gather_runs(grad_out.reshape(run_len, width))

        seg_flat = seg_rows.reshape(-1)
        runs = jnp.stack([c_index, c_index ^ 2, c_index ^ 1, c_index ^ 3])
        ids = (runs[:, None] * run_len + jnp.arange(run_len, dtype=jnp.int32)).reshape(-1)
        before = jnp.sum((seg_flat[None, :] < seg_flat[:, None]).astype(jnp.int32), axis=-1)
        cosine, sine = rope_tables(ids - before)
        allowed = (seg_flat[None, :] == seg_flat[:, None]) & (ids[None, :] <= ids[:, None])
        tokens = ids.shape[0]

        hidden_wide = hidden.astype(jnp.float32)
        attn_normed = (hidden_wide * inverse_rms(hidden_wide) * gains[0]).astype(low)
        projected = dot(attn_normed, full_qkv)
        query = projected[:, :q_cols].reshape(tokens, heads, HEAD_DIM)
        key = projected[:, q_cols : q_cols + kv_cols].reshape(tokens, kv_heads, HEAD_DIM)
        value = projected[:, q_cols + kv_cols :].reshape(tokens, kv_heads, HEAD_DIM)
        query = rotate(query, cosine, sine).astype(low)
        query = query.reshape(tokens, kv_heads, heads // kv_heads, HEAD_DIM)
        key = rotate(key, cosine, sine).astype(low)
        value = value.astype(low)
        scale = HEAD_DIM ** (-0.5)
        scores = (
            jnp.einsum("rkgd,skd->kgrs", query, key, preferred_element_type=jnp.float32) * scale
        )
        scores = jnp.where(allowed, scores, -1e30)
        row_max = jnp.max(scores, axis=-1, keepdims=True)
        row_sum = jnp.sum(jnp.exp(scores - row_max), axis=-1, keepdims=True)
        log_total = row_max + jnp.log(row_sum)
        probs = jnp.exp(scores - log_total)
        prob_low = probs.astype(low)
        attn_rows = jnp.einsum(
            "kgrs,skd->rkgd", prob_low, value, preferred_element_type=jnp.float32
        ).astype(low)
        attn_flat = attn_rows.reshape(tokens, q_cols)

        pair_len = 2 * run_len
        mid = hidden_wide[:pair_len] + reduce_pair(dot(attn_flat, full_out))
        ffn_recip = inverse_rms(mid)
        ffn_scaled = mid * ffn_recip
        ffn_normed = gather_pair((ffn_scaled * gains[1]).astype(low))
        gate_up = dot(ffn_normed, full_gate_up)
        gate, up = gate_up[:, :ff], gate_up[:, ff:]
        sigmoid = jax.nn.sigmoid(gate)
        silu = gate * sigmoid
        inner = (silu * up).astype(low)
        output = (mid[:run_len] + reduce_own(dot(inner, full_down))).astype(low)

        part_down = contract_rows(inner, cotangent).astype(low)
        grad_inner = times_transpose(cotangent, full_down)
        grad_gate = grad_inner * up * sigmoid * (1.0 + gate * (1.0 - sigmoid))
        grad_gate_up = jnp.concatenate(
            [grad_gate.astype(low), (grad_inner * silu).astype(low)], axis=1
        )
        grad_ffn = reduce_pair(times_transpose(grad_gate_up, full_gate_up))
        part_gate_up = contract_rows(ffn_normed, grad_gate_up).astype(low)
        grad_mid = cotangent[:pair_len].astype(jnp.float32) + norm_backward(
            grad_ffn, ffn_scaled, ffn_recip, gains[1]
        )
        ffn_gain_part = jnp.sum(grad_ffn[:run_len] * ffn_scaled[:run_len], axis=0)
        grad_mid_low = gather_pair(grad_mid.astype(low))
        grad_attn = times_transpose(grad_mid_low, full_out).astype(low)
        part_out = contract_rows(attn_flat, grad_mid_low).astype(low)

        grouped = grad_attn.reshape(query.shape)
        grad_probs = jnp.einsum(
            "rkgd,skd->kgrs", grouped, value, preferred_element_type=jnp.float32
        )
        row_delta = jnp.sum(grouped.astype(jnp.float32) * attn_rows.astype(jnp.float32), axis=-1)
        row_delta = jnp.transpose(row_delta, (1, 2, 0))[..., None]
        grad_scores = (probs * (grad_probs - row_delta)).astype(low)
        grad_query = (
            jnp.einsum("kgrs,skd->rkgd", grad_scores, key, preferred_element_type=jnp.float32)
            * scale
        ).reshape(tokens, heads, HEAD_DIM)
        grad_key = (
            jnp.einsum("kgrs,rkgd->skd", grad_scores, query, preferred_element_type=jnp.float32)
            * scale
        )
        grad_value = jnp.einsum(
            "kgrs,rkgd->skd", prob_low, grouped, preferred_element_type=jnp.float32
        )
        grad_qkv = jnp.concatenate(
            [
                rotate_back(grad_query, cosine, sine).astype(low).reshape(tokens, q_cols),
                rotate_back(grad_key, cosine, sine).astype(low).reshape(tokens, kv_cols),
                grad_value.astype(low).reshape(tokens, kv_cols),
            ],
            axis=1,
        )
        part_qkv = contract_rows(attn_normed, grad_qkv).astype(low)
        grad_normed = reduce_own(times_transpose(grad_qkv, full_qkv))
        own_in = hidden_in.reshape(run_len, width).astype(jnp.float32)
        own_recip = inverse_rms(own_in)
        own_scaled = own_in * own_recip
        grad_in = grad_mid[:run_len] + norm_backward(grad_normed, own_scaled, own_recip, gains[0])
        attn_gain_part = jnp.sum(grad_normed * own_scaled, axis=0)

        grad_down = scatter_rows(part_down.reshape(fsdp_size, -1, width), 0)
        grad_gu = scatter_rows(part_gate_up.reshape(ctx_size, fsdp_size, owned, 2 * ff), 1)
        grad_out_w = scatter_rows(part_out.reshape(fsdp_size, -1, width), 0)
        grad_qkv_w = scatter_rows(part_qkv.reshape(ctx_size, fsdp_size, owned, -1), 1)
        grad_gu = spread_columns(grad_gu)
        grad_qkv_w = spread_columns(grad_qkv_w)

        gain_part = jnp.stack([attn_gain_part, ffn_gain_part])
        gain_part = gain_part + to_core(gain_part)
        gain_part = gain_part + to_x(gain_part)
        gain_part = lax.dynamic_index_in_dim(
            gain_part.reshape(2, ctx_size, fsdp_size, owned), c_index, 1, keepdims=False
        )
        gain_own = scatter_rows(gain_part, 1, jnp.float32)

        return (
            output[None],
            grad_in[None],
            grad_qkv_w[:, :, :q_cols].reshape(owned, -1),
            grad_qkv_w[:, :, q_cols : q_cols + kv_cols].reshape(owned, -1),
            grad_qkv_w[:, :, q_cols + kv_cols :].reshape(owned, -1),
            grad_out_w,
            grad_gu[:, :, :ff].reshape(owned, -1),
            grad_gu[:, :, ff:].reshape(owned, -1),
            grad_down,
            gain_own[0],
            gain_own[1],
        )

    return per_device


def solution(mesh):
    rows = P("fsdp", None)
    spread = P(("ctx", "fsdp"), None)
    runs = P("fsdp", "ctx", None)
    return jax.shard_map(
        make_step(mesh.shape["ctx"], mesh.shape["fsdp"]),
        mesh=mesh,
        in_specs=(runs, P("fsdp", "ctx"), *[rows] * 7, P("fsdp"), P("fsdp"), runs),
        out_specs=(runs, runs, *[spread] * 7, P(("ctx", "fsdp")), P(("ctx", "fsdp"))),
        check_vma=False,
    )
```

```python
import functools
import math

import jax
import jax.numpy as jnp
from jax import lax
from jax.experimental import pallas as pl
from jax.experimental.pallas import tpu as pltpu
from jax.sharding import PartitionSpec as P

HEADS = 16
KV_HEADS = 8
HEAD_DIM = 96
EPS = 1e-05
ROPE_BASE = 100000.0

AHEAD = 4
MESH = pl.DeviceIdType.MESH
ANY = pl.BlockSpec(memory_space=pl.ANY)
VMEM = pl.BlockSpec(memory_space=pltpu.VMEM)


def remote(src, dst, send, recv, **where):
    return pltpu.make_async_remote_copy(
        src_ref=src, dst_ref=dst, send_sem=send, recv_sem=recv,
        device_id=where, device_id_type=MESH,
    )


def gather_kernel(ctx_size, fsdp_size, masked, n_blocks, n_runs, *refs):
    depth = fsdp_size // 2
    owns = refs[:n_blocks]
    runs = refs[n_blocks : n_blocks + n_runs]
    fulls = refs[n_blocks + n_runs : 2 * n_blocks + n_runs]
    alls = refs[2 * n_blocks + n_runs : 2 * (n_blocks + n_runs)]
    rest = refs[2 * (n_blocks + n_runs) :]
    stage_blocks, stage_runs = rest[:n_blocks], rest[n_blocks : n_blocks + n_runs]
    z_send, z_recv, y_send, y_recv, c_send, c_recv, local = rest[n_blocks + n_runs :]

    f, c = lax.axis_index("fsdp"), lax.axis_index("ctx")
    z, y = f // 2, f % 2
    span = depth // ctx_size

    barrier = pltpu.get_barrier_semaphore()
    for bits in (1, 2, 3):
        pl.semaphore_signal(barrier, inc=1, device_id={"ctx": c ^ bits}, device_id_type=MESH)
    pl.semaphore_signal(barrier, inc=1, device_id={"fsdp": f ^ 1}, device_id_type=MESH)
    for step in (1, -1):
        near = z + step

        @pl.when((near >= 0) & (near < depth))
        def _():
            pl.semaphore_signal(
                barrier, inc=1, device_id={"fsdp": near * 2 + y}, device_id_type=MESH
            )

    pl.semaphore_wait(barrier, 4 + jnp.minimum(z, 1) + jnp.minimum(depth - 1 - z, 1))

    def held(w, row):
        there = (row >= 0) & (row < depth)
        if masked[w]:
            there = there & (row >= c * span) & (row < (c + 1) * span)
        return there

    def place(w, row, column):
        base = c * span * 2 if masked[w] else 0
        return fulls[w].at[row * 2 + column - base]

    def z_copy(w, way, hop):
        step = 1 if way == 0 else -1
        row = z - step * (hop - 1)
        src = owns[w] if hop == 1 else place(w, row, y)
        near = z + step
        return remote(
            src, place(w, row, y), z_send.at[w, way, hop - 1], z_recv.at[w, way, hop - 1],
            fsdp=near * 2 + y,
        ), held(w, row) & (near >= 0) & (near < depth)

    def y_copy(w, slot, row, own=False):
        src = owns[w] if own else place(w, row, y)
        return remote(
            src, place(w, row, y), y_send.at[w, slot], y_recv.at[w, slot], fsdp=f ^ 1
        ), held(w, row)

    def when_start(pair):
        copy, there = pair
        pl.when(there)(lambda: copy.start())

    def when_sent(pair):
        copy, there = pair
        pl.when(there)(lambda: copy.wait_send())

    for w in range(n_blocks):
        pltpu.make_async_copy(owns[w], stage_blocks[w], local.at[w]).start()
    for r in range(n_runs):
        pltpu.make_async_copy(runs[r], stage_runs[r], local.at[n_blocks + r]).start()
    run_copies = []
    for r in range(n_runs):
        for slot, bits in ((1, 2), (2, 1), (3, 3)):
            copy = remote(
                runs[r], alls[r].at[slot], c_send.at[r, slot - 1], c_recv.at[r, slot - 1],
                ctx=c ^ bits,
            )
            copy.start()
            run_copies.append(copy)
    for w in range(n_blocks):
        when_start(z_copy(w, 0, 1))
        when_start(z_copy(w, 1, 1))
        when_start(y_copy(w, 0, z, own=True))
    for w in range(n_blocks):
        pltpu.make_async_copy(owns[w], stage_blocks[w], local.at[w]).wait()

        @pl.when(held(w, z))
        def _():
            pltpu.make_async_copy(stage_blocks[w], place(w, z, y), local.at[w]).start()

    for r in range(n_runs):
        pltpu.make_async_copy(runs[r], stage_runs[r], local.at[n_blocks + r]).wait()
        pltpu.make_async_copy(stage_runs[r], alls[r].at[0], local.at[n_blocks + r]).start()

    for hop in range(1, depth):
        for w in range(n_blocks):
            for way in (0, 1):
                step = 1 if way == 0 else -1
                row = z - step * hop
                slot = hop if way == 0 else depth - 1 + hop

                @pl.when(held(w, row))
                def _():
                    remote(
                        owns[w], place(w, row, y), z_send.at[w, way, hop - 1],
                        z_recv.at[w, way, hop - 1], fsdp=f ^ 1,
                    ).wait_recv()

                if hop + 1 < depth:
                    when_start(z_copy(w, way, hop + 1))
                when_start(y_copy(w, slot, row))

    for w in range(n_blocks):
        for slot in range(2 * depth - 1):
            row = z - slot if slot < depth else z + (slot - depth + 1)

            @pl.when(held(w, row))
            def _():
                remote(
                    owns[w], place(w, row, 1 - y), y_send.at[w, slot], y_recv.at[w, slot],
                    fsdp=f ^ 1,
                ).wait_recv()

    for copy in run_copies:
        copy.wait()
    for w in range(n_blocks):
        for hop in range(1, depth):
            when_sent(z_copy(w, 0, hop))
            when_sent(z_copy(w, 1, hop))
        for slot in range(2 * depth - 1):
            row = z - slot if slot < depth else z + (slot - depth + 1)
            when_sent(y_copy(w, slot, row, own=slot == 0))

        @pl.when(held(w, z))
        def _():
            pltpu.make_async_copy(stage_blocks[w], place(w, z, y), local.at[w]).wait()

    for r in range(n_runs):
        pltpu.make_async_copy(stage_runs[r], alls[r].at[0], local.at[n_blocks + r]).wait()


def gather_all(ctx_size, fsdp_size, collective_id, blocks, masked, runs):
    depth = fsdp_size // 2
    n_blocks, n_runs = len(blocks), len(runs)
    counts = [fsdp_size // ctx_size if m else fsdp_size for m in masked]
    outs = [jax.ShapeDtypeStruct((n, *b.shape), b.dtype) for n, b in zip(counts, blocks)]
    outs += [jax.ShapeDtypeStruct((ctx_size, *r.shape), r.dtype) for r in runs]
    dma = pltpu.SemaphoreType.DMA
    results = pl.pallas_call(
        functools.partial(gather_kernel, ctx_size, fsdp_size, tuple(masked), n_blocks, n_runs),
        out_shape=tuple(outs),
        in_specs=[ANY] * (n_blocks + n_runs),
        out_specs=(ANY,) * (n_blocks + n_runs),
        scratch_shapes=[
            *[pltpu.VMEM(b.shape, b.dtype) for b in blocks],
            *[pltpu.VMEM(r.shape, r.dtype) for r in runs],
            dma((n_blocks, 2, depth - 1)),
            dma((n_blocks, 2, depth - 1)),
            dma((n_blocks, 2 * depth - 1)),
            dma((n_blocks, 2 * depth - 1)),
            dma((n_runs, 3)),
            dma((n_runs, 3)),
            dma((n_blocks + n_runs,)),
        ],
        compiler_params=pltpu.CompilerParams(
            collective_id=collective_id, has_side_effects=True
        ),
    )(*blocks, *runs)
    return results[:n_blocks], results[n_blocks:]


def add_rows(out_ref, terms, rows):
    total = out_ref.shape[-2]
    chunk = rows if total % rows == 0 else total
    lead = out_ref.shape[0] if len(out_ref.shape) == 3 else None

    def body(step, carry):
        at = pl.ds(pl.multiple_of(step * chunk, chunk), chunk)
        leads = [(at, slice(None))] if lead is None else [(q, at, slice(None)) for q in range(lead)]
        for index in leads:
            value = None
            for ref in terms:
                part = ref[index].astype(jnp.float32)
                value = part if value is None else value + part
            out_ref[index] = value.astype(out_ref.dtype)
        return carry

    lax.fori_loop(0, total // chunk, body, 0)


def scatter_kernel(ctx_size, fsdp_size, kinds, pieces, n, *refs):
    depth = fsdp_size // 2
    parts, gain_part, refs = refs[:n], refs[n], refs[n + 1 :]
    n_out = sum(1 if kind == "rows" else len(piece) for kind, piece in zip(kinds, pieces))
    outs, gain_out, refs = refs[:n_out], refs[n_out], refs[n_out + 1 :]
    own, beside, far, refs = refs[:n], refs[n : 2 * n], refs[2 * n : 3 * n], refs[3 * n :]
    cols = [w for w in range(n) if kinds[w] == "cols"]
    total, block, refs = refs[: len(cols)], refs[len(cols) : 2 * len(cols)], refs[2 * len(cols) :]
    gain_in, gain_ctx, gain_sum, gain_own, gain_beside, gain_far = refs[:6]
    local, y_send, y_recv, z_send, z_recv, c_send, c_recv = refs[6:]

    f, c = lax.axis_index("fsdp"), lax.axis_index("ctx")
    z, y = f // 2, f % 2

    barrier = pltpu.get_barrier_semaphore()
    for bits in (1, 2, 3):
        pl.semaphore_signal(barrier, inc=1, device_id={"ctx": c ^ bits}, device_id_type=MESH)
    pl.semaphore_signal(barrier, inc=1, device_id={"fsdp": f ^ 1}, device_id_type=MESH)
    for step in (1, -1):
        near = z + step

        @pl.when((near >= 0) & (near < depth))
        def _():
            pl.semaphore_signal(
                barrier, inc=1, device_id={"fsdp": near * 2 + y}, device_id_type=MESH
            )

    pl.semaphore_wait(barrier, 4 + jnp.minimum(z, 1) + jnp.minimum(depth - 1 - z, 1))

    order = []
    for t in range((depth + 1) // 2):
        order += [depth - 1 - t, t] if depth - 1 - t != t else [t]

    def chunk(w, row, column):
        at = row * 2 + column
        return parts[w].at[at] if kinds[w] == "rows" else parts[w].at[:, at]

    def y_copy(w, t):
        if w == n:
            src, dst = gain_sum.at[t * 2 + 1 - y], gain_beside.at[t]
        else:
            src, dst = chunk(w, t, 1 - y), beside[w].at[t]
        return remote(src, dst, y_send.at[w, t], y_recv.at[w, t], fsdp=f ^ 1)

    def z_copy(w, t, step, slot):
        held, arrived = (gain_own, gain_far) if w == n else (own[w], far[w])
        return remote(
            held.at[t], arrived.at[slot], z_send.at[w, t], z_recv.at[w, slot],
            fsdp=(z + step) * 2 + y,
        )

    def own_copy(w, t):
        return pltpu.make_async_copy(chunk(w, t, y), own[w].at[t], local.at[w, t])

    def add_into(w, t, ref):
        if w == n:
            gain_own[t] = gain_own[t] + ref[...]
        else:
            add_rows(own[w].at[t], (own[w].at[t], ref), 16)

    def pass_on(w, t):
        arrived = gain_far if w == n else far[w]
        beside_t = gain_beside.at[t] if w == n else beside[w].at[t]
        for step in (1, -1):
            ahead = (t - z) * step
            behind = (z - step >= 0) & (z - step < depth)

            @pl.when((ahead > 0) & behind)
            def _():
                z_copy(w, t, step, t).wait_recv()
                if w == n:
                    gain_own[t] = gain_own[t] + beside_t[...] + arrived[t]
                else:
                    add_rows(own[w].at[t], (own[w].at[t], beside_t, arrived.at[t]), 16)

            @pl.when((ahead > 0) & jnp.logical_not(behind))
            def _():
                if w == n:
                    gain_own[t] = gain_own[t] + beside_t[...]
                else:
                    add_rows(own[w].at[t], (own[w].at[t], beside_t), 16)

            slot = t if step == 1 else t + jnp.where(ahead == 1, depth - t, 0)

            @pl.when(ahead > 0)
            def _():
                z_copy(w, t, step, slot).start()

    def sent(w, t):
        for step in (1, -1):

            @pl.when((t - z) * step > 0)
            def _():
                z_copy(w, t, step, t).wait_send()

    def come_home(w):
        @pl.when(z > 0)
        def _():
            z_copy(w, 0, 1, z).wait_recv()

        @pl.when(z < depth - 1)
        def _():
            z_copy(w, 0, 1, depth).wait_recv()

    def c_copy(k, bits):
        if k == len(cols):
            src, dst = gain_part.at[c ^ bits], gain_ctx.at[bits - 1]
        else:
            src, dst = total[k].at[c ^ bits], block[k].at[bits - 1]
        return remote(
            src, dst, c_send.at[k, bits - 1], c_recv.at[k, bits - 1], ctx=c ^ bits
        )

    gain_local = pltpu.make_async_copy(gain_part.at[c], gain_in, local.at[n, 0])
    gain_local.start()
    for bits in (1, 2, 3):
        c_copy(len(cols), bits).start()
    sequence = [(w, t) for w in range(n) for t in order]
    for w, t in sequence[:AHEAD]:
        y_copy(w, t).start()
    for w, t in sequence:
        own_copy(w, t).start()

    gain_local.wait()
    for bits in (1, 2, 3):
        c_copy(len(cols), bits).wait()
    gain_sum[...] = gain_in[...] + gain_ctx[0] + gain_ctx[1] + gain_ctx[2]
    for t in order:
        y_copy(n, t).start()

    def reduce_beside(w):
        for t in order:
            if w == n:
                gain_own[t] = gain_sum[t * 2 + y]
            else:
                own_copy(w, t).wait()
            y_copy(w, t).wait_recv()
            if w < n:
                later = w * depth + order.index(t) + AHEAD
                if later < len(sequence):
                    y_copy(*sequence[later]).start()
            pass_on(w, t)

    def first_out(w):
        return sum(1 if kinds[v] == "rows" else len(pieces[v]) for v in range(w))

    def finish(w):
        come_home(w)
        if w == n:
            target = gain_out
            home = [gain_own.at[z], gain_beside.at[z]]
            ends = [gain_far.at[z], gain_far.at[depth]]
        else:
            target = outs[first_out(w)] if kinds[w] == "rows" else total[cols.index(w)]
            home = [own[w].at[z], beside[w].at[z]]
            ends = [far[w].at[z], far[w].at[depth]]

        @pl.when(z == 0)
        def _():
            add_rows(target, (*home, ends[1]), 16)

        @pl.when(z == depth - 1)
        def _():
            add_rows(target, (*home, ends[0]), 16)

        @pl.when((z > 0) & (z < depth - 1))
        def _():
            add_rows(target, (*home, *ends), 16)

        if w < n and kinds[w] == "cols":
            for bits in (1, 2, 3):
                c_copy(cols.index(w), bits).start()

    def spread(w):
        k = cols.index(w)
        first = first_out(w)
        for bits in (0, 1, 2, 3):
            if bits:
                c_copy(k, bits).wait_recv()
            source = total[k].at[c] if bits == 0 else block[k].at[bits - 1]
            at = 0
            for j, (size, flat) in enumerate(pieces[w]):
                value = source[:, at : at + size].astype(jnp.float32)
                if flat:
                    where = pl.ds(pl.multiple_of((c ^ bits) * size, 128), size)
                    outs[first + j][:, where] = value
                else:
                    outs[first + j][c ^ bits] = value
                at += size

    for w in range(n):
        reduce_beside(w)
        if w == 0:
            reduce_beside(n)
        else:
            finish(w - 1)
    for w in cols:
        if w < n - 1:
            spread(w)
    finish(n - 1)
    if n - 1 in cols:
        spread(n - 1)
    finish(n)

    for w in range(n + 1):
        for t in order:
            y_copy(w, t).wait_send()
            sent(w, t)
    for k in range(len(cols)):
        for bits in (1, 2, 3):
            c_copy(k, bits).wait_send()


def scatter_all(ctx_size, fsdp_size, collective_id, parts, kinds, pieces, gains):
    depth = fsdp_size // 2
    n = len(parts)
    outs, chunks = [], []
    for part, kind, piece in zip(parts, kinds, pieces):
        if kind == "rows":
            chunks.append(part.shape[1:])
            outs.append(jax.ShapeDtypeStruct(part.shape[1:], jnp.float32))
            continue
        chunks.append((part.shape[0], *part.shape[2:]))
        rows = part.shape[2]
        for size, flat in piece:
            shape = (rows, ctx_size * size) if flat else (ctx_size, rows, size)
            outs.append(jax.ShapeDtypeStruct(shape, jnp.float32))
    outs.append(jax.ShapeDtypeStruct((8, 128), jnp.float32))
    wide = [chunk for chunk, kind in zip(chunks, kinds) if kind == "cols"]
    low, dma = jnp.bfloat16, pltpu.SemaphoreType.DMA
    tile = (8, 128)
    return pl.pallas_call(
        functools.partial(scatter_kernel, ctx_size, fsdp_size, tuple(kinds), tuple(pieces), n),
        out_shape=tuple(outs),
        in_specs=[ANY] * (n + 1),
        out_specs=(VMEM,) * len(outs),
        scratch_shapes=[
            *[pltpu.VMEM((depth, *chunk), low) for chunk in chunks],
            *[pltpu.VMEM((depth, *chunk), low) for chunk in chunks],
            *[pltpu.VMEM((depth + 1, *chunk), low) for chunk in chunks],
            *[pltpu.VMEM(chunk, low) for chunk in wide],
            *[pltpu.VMEM((3, *chunk[1:]), low) for chunk in wide],
            pltpu.VMEM((fsdp_size, *tile), jnp.float32),
            pltpu.VMEM((3, fsdp_size, *tile), jnp.float32),
            pltpu.VMEM((fsdp_size, *tile), jnp.float32),
            pltpu.VMEM((depth, *tile), jnp.float32),
            pltpu.VMEM((depth, *tile), jnp.float32),
            pltpu.VMEM((depth + 1, *tile), jnp.float32),
            dma((n + 1, depth)),
            dma((n + 1, depth)),
            dma((n + 1, depth)),
            dma((n + 1, depth)),
            dma((n + 1, depth + 1)),
            dma((len(wide) + 1, 3)),
            dma((len(wide) + 1, 3)),
        ],
        compiler_params=pltpu.CompilerParams(
            collective_id=collective_id, has_side_effects=True, vmem_limit_bytes=50 * 2**20
        ),
    )(*parts, gains)


def inverse_rms(values):
    return lax.rsqrt(jnp.mean(values * values, axis=-1, keepdims=True) + EPS)


def norm_backward(grad_normed, scaled, inv_rms, gain):
    grad_scaled = grad_normed * gain
    return inv_rms * (
        grad_scaled - scaled * jnp.mean(grad_scaled * scaled, axis=-1, keepdims=True)
    )


def rope_tables(positions):
    half_dim = HEAD_DIM // 2
    freq_index = jnp.arange(half_dim, dtype=jnp.float32)
    frequency = jnp.exp(freq_index * (-2.0 / HEAD_DIM) * math.log(ROPE_BASE))
    angles = positions.astype(jnp.float32)[:, None] * frequency
    return (jnp.cos(angles)[:, None, :], jnp.sin(angles)[:, None, :])


def rotate(tensor, cosine, sine):
    half_dim = tensor.shape[-1] // 2
    front, back = tensor[..., :half_dim], tensor[..., half_dim:]
    return jnp.concatenate([front * cosine - back * sine, back * cosine + front * sine], axis=-1)


def rotate_back(tensor, cosine, sine):
    return rotate(tensor, cosine, -sine)


def dot(left, right):
    return jnp.dot(left, right, preferred_element_type=jnp.float32)


def contract_rows(left, right):
    return lax.dot_general(
        left, right, (((0,), (0,)), ((), ())), preferred_element_type=jnp.float32
    )


def times_transpose(left, weight):
    return lax.dot_general(
        left, weight, (((1,), (1,)), ((), ())), preferred_element_type=jnp.float32
    )


def make_step(ctx_size, fsdp_size):
    depth = fsdp_size // 2
    low = jnp.bfloat16

    core_pairs = [(c, c ^ 1) for c in range(ctx_size)]
    x_pairs = [(c, c ^ 2) for c in range(ctx_size)]
    def to_core(value):
        return lax.ppermute(value, "ctx", core_pairs)

    def to_x(value):
        return lax.ppermute(value, "ctx", x_pairs)

    def gather_pair(pair):
        return jnp.concatenate([pair, to_core(pair)], axis=0)

    def reduce_core(partial):
        half = partial.shape[0] // 2
        received = to_core(partial[half:].astype(low))
        return partial[:half] + received.astype(jnp.float32)

    def reduce_pair(partial):
        pair = reduce_core(partial).astype(low)
        other = to_x(pair)
        half = pair.shape[0] // 2
        other = jnp.concatenate([other[half:], other[:half]], axis=0)
        return pair.astype(jnp.float32) + other.astype(jnp.float32)

    def reduce_own(partial):
        pair = reduce_core(partial)
        half = pair.shape[0] // 2
        return pair[:half] + to_x(pair[half:].astype(low)).astype(jnp.float32)

    def per_device(
        hidden_in,
        segments,
        w_query,
        w_key,
        w_value,
        w_out,
        w_gate,
        w_up,
        w_down,
        attn_gain,
        ffn_gain,
        grad_out,
    ):
        _, run_len, width = hidden_in.shape
        c_index = lax.axis_index("ctx")
        heads, kv_heads = HEADS // ctx_size, KV_HEADS // ctx_size
        q_cols, kv_cols = heads * HEAD_DIM, kv_heads * HEAD_DIM
        ff = w_gate.shape[1] // ctx_size
        shard = width // fsdp_size
        owned = shard // ctx_size

        def columns(weight, size):
            return lax.dynamic_slice_in_dim(weight, c_index * size, size, 1)

        lanes = -shard % 128
        blocks, (hidden, cotangent, seg_rows) = gather_all(
            ctx_size,
            fsdp_size,
            0,
            (
                jnp.concatenate(
                    [columns(w_query, q_cols), columns(w_key, kv_cols), columns(w_value, kv_cols)],
                    axis=1,
                ),
                jnp.concatenate([columns(w_gate, ff), columns(w_up, ff)], axis=1),
                w_out,
                w_down,
                jnp.pad(jnp.stack([attn_gain, ffn_gain]), ((0, 6), (0, lanes))),
            ),
            (False, False, True, True, False),
            (
                hidden_in.reshape(run_len, width),
                grad_out.reshape(run_len, width),
                jnp.broadcast_to(segments, (8, run_len)),
            ),
        )
        full_qkv = blocks[0].reshape(width, q_cols + 2 * kv_cols)
        full_gate_up = blocks[1].reshape(width, 2 * ff)
        full_out = blocks[2].reshape(q_cols, width)
        full_down = blocks[3].reshape(ff, width)
        gains = jnp.swapaxes(blocks[4][:, :2, :shard], 0, 1).reshape(2, width).astype(jnp.float32)
        hidden = hidden.reshape(-1, width)
        cotangent = cotangent.reshape(-1, width)

        seg_flat = seg_rows[:, 0].reshape(-1)
        runs = jnp.stack([c_index, c_index ^ 2, c_index ^ 1, c_index ^ 3])
        ids = (runs[:, None] * run_len + jnp.arange(run_len, dtype=jnp.int32)).reshape(-1)
        before = jnp.sum((seg_flat[None, :] < seg_flat[:, None]).astype(jnp.int32), axis=-1)
        cosine, sine = rope_tables(ids - before)
        allowed = (seg_flat[None, :] == seg_flat[:, None]) & (ids[None, :] <= ids[:, None])
        tokens = ids.shape[0]

        hidden_wide = hidden.astype(jnp.float32)
        attn_normed = (hidden_wide * inverse_rms(hidden_wide) * gains[0]).astype(low)
        projected = dot(attn_normed, full_qkv)
        query = projected[:, :q_cols].reshape(tokens, heads, HEAD_DIM)
        key = projected[:, q_cols : q_cols + kv_cols].reshape(tokens, kv_heads, HEAD_DIM)
        value = projected[:, q_cols + kv_cols :].reshape(tokens, kv_heads, HEAD_DIM)
        query = rotate(query, cosine, sine).astype(low)
        query = query.reshape(tokens, kv_heads, heads // kv_heads, HEAD_DIM)
        key = rotate(key, cosine, sine).astype(low)
        value = value.astype(low)
        scale = HEAD_DIM ** (-0.5)
        scores = (
            jnp.einsum("rkgd,skd->kgrs", query, key, preferred_element_type=jnp.float32) * scale
        )
        scores = jnp.where(allowed, scores, -1e30)
        row_max = jnp.max(scores, axis=-1, keepdims=True)
        row_sum = jnp.sum(jnp.exp(scores - row_max), axis=-1, keepdims=True)
        log_total = row_max + jnp.log(row_sum)
        probs = jnp.exp(scores - log_total)
        prob_low = probs.astype(low)
        attn_rows = jnp.einsum(
            "kgrs,skd->rkgd", prob_low, value, preferred_element_type=jnp.float32
        ).astype(low)
        attn_flat = attn_rows.reshape(tokens, q_cols)

        pair_len = 2 * run_len
        mid = hidden_wide[:pair_len] + reduce_pair(dot(attn_flat, full_out))
        ffn_recip = inverse_rms(mid)
        ffn_scaled = mid * ffn_recip
        ffn_normed = gather_pair((ffn_scaled * gains[1]).astype(low))
        gate_up = dot(ffn_normed, full_gate_up)
        gate, up = gate_up[:, :ff], gate_up[:, ff:]
        sigmoid = jax.nn.sigmoid(gate)
        silu = gate * sigmoid
        inner = (silu * up).astype(low)
        output = (mid[:run_len] + reduce_own(dot(inner, full_down))).astype(low)

        part_down = contract_rows(inner, cotangent).astype(low)
        grad_inner = times_transpose(cotangent, full_down)
        grad_gate = grad_inner * up * sigmoid * (1.0 + gate * (1.0 - sigmoid))
        grad_gate_up = jnp.concatenate(
            [grad_gate.astype(low), (grad_inner * silu).astype(low)], axis=1
        )
        grad_ffn = reduce_pair(times_transpose(grad_gate_up, full_gate_up))
        part_gate_up = contract_rows(ffn_normed, grad_gate_up).astype(low)
        grad_mid = cotangent[:pair_len].astype(jnp.float32) + norm_backward(
            grad_ffn, ffn_scaled, ffn_recip, gains[1]
        )
        ffn_gain_part = jnp.sum(grad_ffn[:run_len] * ffn_scaled[:run_len], axis=0)
        grad_mid_low = gather_pair(grad_mid.astype(low))
        grad_attn = times_transpose(grad_mid_low, full_out).astype(low)
        part_out = contract_rows(attn_flat, grad_mid_low).astype(low)

        grouped = grad_attn.reshape(query.shape)
        grad_probs = jnp.einsum(
            "rkgd,skd->kgrs", grouped, value, preferred_element_type=jnp.float32
        )
        row_delta = jnp.sum(grouped.astype(jnp.float32) * attn_rows.astype(jnp.float32), axis=-1)
        row_delta = jnp.transpose(row_delta, (1, 2, 0))[..., None]
        grad_scores = (probs * (grad_probs - row_delta)).astype(low)
        grad_query = (
            jnp.einsum("kgrs,skd->rkgd", grad_scores, key, preferred_element_type=jnp.float32)
            * scale
        ).reshape(tokens, heads, HEAD_DIM)
        grad_key = (
            jnp.einsum("kgrs,rkgd->skd", grad_scores, query, preferred_element_type=jnp.float32)
            * scale
        )
        grad_value = jnp.einsum(
            "kgrs,rkgd->skd", prob_low, grouped, preferred_element_type=jnp.float32
        )
        grad_qkv = jnp.concatenate(
            [
                rotate_back(grad_query, cosine, sine).astype(low).reshape(tokens, q_cols),
                rotate_back(grad_key, cosine, sine).astype(low).reshape(tokens, kv_cols),
                grad_value.astype(low).reshape(tokens, kv_cols),
            ],
            axis=1,
        )
        part_qkv = contract_rows(attn_normed, grad_qkv).astype(low)
        grad_normed = reduce_own(times_transpose(grad_qkv, full_qkv))
        own_in = hidden_in.reshape(run_len, width).astype(jnp.float32)
        own_recip = inverse_rms(own_in)
        own_scaled = own_in * own_recip
        grad_in = grad_mid[:run_len] + norm_backward(grad_normed, own_scaled, own_recip, gains[0])
        attn_gain_part = jnp.sum(grad_normed * own_scaled, axis=0)

        gain_part = jnp.stack([attn_gain_part, ffn_gain_part])
        gain_part = gain_part.reshape(2, ctx_size, fsdp_size, owned).transpose(1, 2, 0, 3)
        gain_part = jnp.pad(gain_part, ((0, 0), (0, 0), (0, 6), (0, 128 - owned)))
        grad_gate_w, grad_up_w, grad_query_w, grad_kv_w, grad_down_w, grad_out_w, gains_own = (
            scatter_all(
                ctx_size,
                fsdp_size,
                1,
                (
                    part_gate_up.reshape(ctx_size, fsdp_size, owned, 2 * ff),
                    part_qkv.reshape(ctx_size, fsdp_size, owned, -1),
                    part_down.reshape(fsdp_size, -1, width),
                    part_out.reshape(fsdp_size, -1, width),
                ),
                ("cols", "cols", "rows", "rows"),
                (
                    ((ff, True), (ff, True)),
                    ((q_cols, True), (2 * kv_cols, False)),
                    None,
                    None,
                ),
                gain_part,
            )
        )
        grad_kv_w = jnp.swapaxes(grad_kv_w, 0, 1)

        return (
            output[None],
            grad_in[None],
            grad_query_w,
            grad_kv_w[:, :, :kv_cols].reshape(owned, -1),
            grad_kv_w[:, :, kv_cols:].reshape(owned, -1),
            grad_out_w,
            grad_gate_w,
            grad_up_w,
            grad_down_w,
            gains_own[0, :owned],
            gains_own[1, :owned],
        )

    return per_device


def solution(mesh):
    rows = P("fsdp", None)
    spread = P(("ctx", "fsdp"), None)
    runs = P("fsdp", "ctx", None)
    return jax.shard_map(
        make_step(mesh.shape["ctx"], mesh.shape["fsdp"]),
        mesh=mesh,
        in_specs=(runs, P("fsdp", "ctx"), *[rows] * 7, P("fsdp"), P("fsdp"), runs),
        out_specs=(runs, runs, *[spread] * 7, P(("ctx", "fsdp")), P(("ctx", "fsdp"))),
        check_vma=False,
    )
```

```python
import functools
import math

import jax
import jax.numpy as jnp
from jax import lax
from jax.experimental import pallas as pl
from jax.experimental.pallas import tpu as pltpu
from jax.sharding import PartitionSpec as P

HEADS = 16
KV_HEADS = 8
HEAD_DIM = 96
EPS = 1e-05
ROPE_BASE = 100000.0

AHEAD = 4
MESH = pl.DeviceIdType.MESH
ANY = pl.BlockSpec(memory_space=pl.ANY)
VMEM = pl.BlockSpec(memory_space=pltpu.VMEM)
DMA = pltpu.SemaphoreType.DMA
LOW = jnp.bfloat16
WIDE = jnp.float32


def remote(src, dst, send, recv, **where):
    return pltpu.make_async_remote_copy(
        src_ref=src,
        dst_ref=dst,
        send_sem=send,
        recv_sem=recv,
        device_id=where,
        device_id_type=MESH,
    )


def place(fsdp_size):
    f, c = lax.axis_index("fsdp"), lax.axis_index("ctx")
    return f, c, f // 2, f % 2, fsdp_size // 2


def greet(fsdp_size):
    f, c, z, y, depth = place(fsdp_size)
    barrier = pltpu.get_barrier_semaphore()
    for bits in (1, 2, 3):
        pl.semaphore_signal(barrier, inc=1, device_id={"ctx": c ^ bits}, device_id_type=MESH)
    pl.semaphore_signal(barrier, inc=1, device_id={"fsdp": f ^ 1}, device_id_type=MESH)
    for step in (1, -1):
        near = z + step

        @pl.when((near >= 0) & (near < depth))
        def _():
            pl.semaphore_signal(
                barrier, inc=1, device_id={"fsdp": near * 2 + y}, device_id_type=MESH
            )

    pl.semaphore_wait(barrier, 4 + jnp.minimum(z, 1) + jnp.minimum(depth - 1 - z, 1))


class LineGather:
    def __init__(self, ctx_size, fsdp_size, masked, blocks, owns, fulls, stages, sems):
        self.sizes = ctx_size, fsdp_size
        self.f, self.c, self.z, self.y, self.depth = place(fsdp_size)
        self.masked, self.blocks = masked, blocks
        self.owns, self.fulls, self.stages = owns, fulls, stages
        self.z_send, self.z_recv, self.y_send, self.y_recv, self.local = sems
        self.beside_done = set()

    @staticmethod
    def scratch(fsdp_size, arrays, count):
        depth = fsdp_size // 2
        return [
            *[pltpu.VMEM(a.shape, a.dtype) for a in arrays],
            DMA((count, 2, depth - 1)),
            DMA((count, 2, depth - 1)),
            DMA((count, 2 * depth - 1)),
            DMA((count, 2 * depth - 1)),
            DMA((len(arrays),)),
        ]

    def held(self, a, row):
        there = (row >= 0) & (row < self.depth)
        if self.masked[a]:
            span = self.depth // self.sizes[0]
            there = there & (row >= self.c * span) & (row < (self.c + 1) * span)
        return there

    def entry(self, a, row, column):
        base = self.c * (self.sizes[1] // self.sizes[0]) if self.masked[a] else 0
        return row * 2 + column - base

    def spot(self, b, row, column):
        a, low, size = self.blocks[b]
        return self.fulls[a].at[self.entry(a, row, column), pl.ds(low, size)]

    def source(self, b, row):
        a, low, size = self.blocks[b]
        return self.owns[a].at[pl.ds(low, size)] if row is None else self.spot(b, row, self.y)

    def z_copy(self, b, way, hop):
        step = 1 if way == 0 else -1
        row = self.z - step * (hop - 1)
        near = self.z + step
        copy = remote(
            self.source(b, None if hop == 1 else row),
            self.spot(b, row, self.y),
            self.z_send.at[b, way, hop - 1],
            self.z_recv.at[b, way, hop - 1],
            fsdp=near * 2 + self.y,
        )
        return copy, self.held(self.blocks[b][0], row) & (near >= 0) & (near < self.depth)

    def row_of(self, slot):
        return self.z - slot if slot < self.depth else self.z + (slot - self.depth + 1)

    def y_copy(self, b, slot):
        row = self.row_of(slot)
        copy = remote(
            self.source(b, row if slot else None),
            self.spot(b, row, self.y),
            self.y_send.at[b, slot],
            self.y_recv.at[b, slot],
            fsdp=self.f ^ 1,
        )
        return copy, self.held(self.blocks[b][0], row)

    @staticmethod
    def begin(pair):
        pl.when(pair[1])(lambda: pair[0].start())

    def send_own(self, b):
        self.begin(self.z_copy(b, 0, 1))
        self.begin(self.z_copy(b, 1, 1))
        self.begin(self.y_copy(b, 0))

    def local_in(self, a):
        return pltpu.make_async_copy(self.owns[a], self.stages[a], self.local.at[a])

    def local_out(self, a):
        spot = self.fulls[a].at[self.entry(a, self.z, self.y)]
        return pltpu.make_async_copy(self.stages[a], spot, self.local.at[a])

    def start(self):
        for a in range(len(self.owns)):
            self.local_in(a).start()
        for b in range(min(2, len(self.blocks))):
            self.send_own(b)
        for a in range(len(self.owns)):
            self.local_in(a).wait()
            pl.when(self.held(a, self.z))(lambda a=a: self.local_out(a).start())

    def step(self, b, hop):
        a = self.blocks[b][0]
        for way in (0, 1):
            row = self.z - hop if way == 0 else self.z + hop

            @pl.when(self.held(a, row))
            def _():
                remote(
                    self.source(b, None),
                    self.spot(b, row, self.y),
                    self.z_send.at[b, way, hop - 1],
                    self.z_recv.at[b, way, hop - 1],
                    fsdp=self.f ^ 1,
                ).wait_recv()

            if hop + 1 < self.depth:
                self.begin(self.z_copy(b, way, hop + 1))
            self.begin(self.y_copy(b, hop if way == 0 else self.depth - 1 + hop))
        if hop == 1 and b + 2 < len(self.blocks):
            self.send_own(b + 2)

    def steps(self):
        return [
            functools.partial(self.step, b, hop)
            for b in range(len(self.blocks))
            for hop in range(1, self.depth)
        ]

    def wait_local(self, a):
        pl.when(self.held(a, self.z))(lambda: self.local_out(a).wait())

    def wait_beside(self, b):
        if b in self.beside_done:
            return
        self.beside_done.add(b)
        for slot in range(2 * self.depth - 1):
            row = self.row_of(slot)

            @pl.when(self.held(self.blocks[b][0], row))
            def _():
                remote(
                    self.source(b, None),
                    self.spot(b, row, 1 - self.y),
                    self.y_send.at[b, slot],
                    self.y_recv.at[b, slot],
                    fsdp=self.f ^ 1,
                ).wait_recv()

    def finish(self, local_done=()):
        for b in range(len(self.blocks)):
            self.wait_beside(b)
        pairs = []
        for b in range(len(self.blocks)):
            for hop in range(1, self.depth):
                pairs += [self.z_copy(b, 0, hop), self.z_copy(b, 1, hop)]
            pairs += [self.y_copy(b, slot) for slot in range(2 * self.depth - 1)]
        for copy, there in pairs:
            pl.when(there)(lambda copy=copy: copy.wait_send())
        for a in range(len(self.owns)):
            if a not in local_done:
                self.wait_local(a)


def weave(steps, inserts):
    for i, step in enumerate(steps):
        for extra in inserts.get(i, ()):
            extra()
        step()
    for i in sorted(inserts):
        if i >= len(steps):
            for extra in inserts[i]:
                extra()


def row_loop(total, body, rows=16):
    rows = rows if total % rows == 0 else total

    def run(step, carry):
        body(pl.ds(pl.multiple_of(step * rows, rows), rows))
        return carry

    lax.fori_loop(0, total // rows, run, 0)


def add_rows(out_ref, terms):
    shape = out_ref.shape
    leads = [None] if len(shape) == 2 else list(range(shape[0]))

    def body(at):
        for lead in leads:
            index = (at,) if lead is None else (lead, at)
            value = None
            for ref in terms:
                part = ref[index].astype(WIDE)
                value = part if value is None else value + part
            out_ref[index] = value.astype(out_ref.dtype)

    row_loop(shape[-2], body)


def first_kernel(ctx_size, fsdp_size, n_blocks, n_runs, *refs):
    owns, runs, refs = refs[:n_blocks], refs[n_blocks : n_blocks + n_runs], refs[n_blocks + n_runs :]
    fulls, alls, refs = refs[:n_blocks], refs[n_blocks : n_blocks + n_runs], refs[n_blocks + n_runs :]
    stages, sems, refs = refs[:n_blocks], refs[n_blocks : n_blocks + 5], refs[n_blocks + 5 :]
    stage_runs, (c_send, c_recv, local) = refs[:n_runs], refs[n_runs:]
    c = lax.axis_index("ctx")
    blocks = [(a, 0, owns[a].shape[0]) for a in range(n_blocks)]
    line = LineGather(
        ctx_size, fsdp_size, (False,) * n_blocks, blocks, owns, fulls, stages, sems
    )
    greet(fsdp_size)

    def run_copy(r, bits):
        slot = (0, 2, 1, 3)[bits]
        return remote(
            runs[r], alls[r].at[slot], c_send.at[r, bits - 1], c_recv.at[r, bits - 1], ctx=c ^ bits
        )

    line.start()
    for r in range(n_runs):
        pltpu.make_async_copy(runs[r], stage_runs[r], local.at[r]).start()
        for bits in (2, 1, 3):
            run_copy(r, bits).start()
    for r in range(n_runs):
        pltpu.make_async_copy(runs[r], stage_runs[r], local.at[r]).wait()
        pltpu.make_async_copy(stage_runs[r], alls[r].at[0], local.at[r]).start()
    weave(line.steps(), {})
    line.finish()
    for r in range(n_runs):
        for bits in (2, 1, 3):
            run_copy(r, bits).wait()
        pltpu.make_async_copy(stage_runs[r], alls[r].at[0], local.at[r]).wait()


def gather_first(ctx_size, fsdp_size, collective_id, blocks, runs):
    n_blocks, n_runs = len(blocks), len(runs)
    outs = [jax.ShapeDtypeStruct((fsdp_size, *b.shape), b.dtype) for b in blocks]
    outs += [jax.ShapeDtypeStruct((ctx_size, *r.shape), r.dtype) for r in runs]
    results = pl.pallas_call(
        functools.partial(first_kernel, ctx_size, fsdp_size, n_blocks, n_runs),
        out_shape=tuple(outs),
        in_specs=[ANY] * (n_blocks + n_runs),
        out_specs=(ANY,) * (n_blocks + n_runs),
        scratch_shapes=[
            *LineGather.scratch(fsdp_size, blocks, n_blocks),
            *[pltpu.VMEM(r.shape, r.dtype) for r in runs],
            DMA((n_runs, 3)),
            DMA((n_runs, 3)),
            DMA((n_runs,)),
        ],
        compiler_params=pltpu.CompilerParams(collective_id=collective_id, has_side_effects=True),
    )(*blocks, *runs)
    return results[:n_blocks], results[n_blocks:]


def second_kernel(ctx_size, fsdp_size, blocks, heads, kv_heads, *refs):
    owns, refs = refs[:3], refs[3:]
    query, key, value, bias, hidden, gain, refs = *refs[:6], refs[6:]
    fulls, refs = refs[:3], refs[3:]
    rows_out, log_out, mid_out, normed, refs = *refs[:4], refs[4:]
    stages, sems, refs = refs[:3], refs[3:8], refs[8:]
    w_pad, kept, core_out, core_in, pair, pair_in, c_send, c_recv, w_sem = refs
    c = lax.axis_index("ctx")
    line = LineGather(ctx_size, fsdp_size, (True, False, True), blocks, owns, fulls, stages, sems)
    tokens, half = query.shape[1], hidden.shape[0]
    run_len = half // 2
    scale = HEAD_DIM**-0.5
    tile = 128

    def attention(part):
        def body(i, carry):
            h = i // (tokens // tile)
            r = i % (tokens // tile)
            at = pl.ds(pl.multiple_of(r * tile, tile), tile)
            g = h // (heads // kv_heads)
            s = lax.dot_general(
                query[h, at], key[g], (((1,), (1,)), ((), ())), preferred_element_type=WIDE
            )
            s = s * scale + bias[at]
            top = jnp.max(s, axis=-1, keepdims=True)
            log = top + jnp.log(jnp.sum(jnp.exp(s - top), axis=-1, keepdims=True))
            p = jnp.exp(s - log).astype(LOW)
            mixed = jnp.dot(p, value[g], preferred_element_type=WIDE)
            rows_out[at, pl.ds(pl.multiple_of(h * 128, 128), 128)] = mixed.astype(LOW)
            log_out[h, at] = log
            return carry

        count = heads * (tokens // tile)
        lax.fori_loop(part * count // 2, (part + 1) * count // 2, body, 0)

    def exchange(index, src, dst, bits):
        return remote(src, dst, c_send.at[index], c_recv.at[index], ctx=c ^ bits)

    to_core = exchange(0, core_out, core_in, 1)
    to_x = exchange(1, pair, pair_in, 2)
    give = exchange(2, normed.at[pl.ds(0, half)], normed.at[pl.ds(half, half)], 1)

    shard = owns[0].shape[0]
    piece = min(shard, HEAD_DIM)
    moves = []
    for at in range(0, heads * HEAD_DIM, piece):
        to = at // HEAD_DIM * 128 + at % HEAD_DIM
        src = fulls[0].at[at // shard, pl.ds(at % shard, piece)]
        moves.append(pltpu.make_async_copy(src, w_pad.at[pl.ds(to, piece)], w_sem.at[len(moves)]))

    def load_out():
        line.wait_beside(0)
        line.wait_local(0)
        for move in moves:
            move.start()
        for h in range(heads):
            w_pad[pl.ds(h * 128 + HEAD_DIM, 128 - HEAD_DIM)] = jnp.zeros(
                (128 - HEAD_DIM, w_pad.shape[1]), LOW
            )
        for move in moves:
            move.wait()

    def project():
        def far(at):
            value_rows = rows_out[pl.ds(pl.multiple_of(at.start + half, tile), tile)]
            core_out[at] = jnp.dot(value_rows, w_pad[...], preferred_element_type=WIDE).astype(LOW)

        row_loop(half, far, tile)
        to_core.start()

        def near(at):
            kept[at] = jnp.dot(rows_out[at], w_pad[...], preferred_element_type=WIDE)

        row_loop(half, near, tile)

    def meet_core():
        to_core.wait_recv()
        add_rows(pair, (kept, core_in))
        to_x.start()

    def meet_x():
        to_x.wait_recv()
        for block in (0, 1):

            def body(at, block=block):
                here = pl.ds(pl.multiple_of(at.start + block * run_len, 16), 16)
                there = pl.ds(pl.multiple_of(at.start + (1 - block) * run_len, 16), 16)
                mid = hidden[here].astype(WIDE) + (
                    pair[here].astype(WIDE) + pair_in[there].astype(WIDE)
                )
                mid_out[here] = mid
                scaled = mid * inverse_rms(mid)
                normed[here] = (scaled * gain[0:1]).astype(LOW)

            row_loop(run_len, body)
        give.start()

    greet(fsdp_size)
    line.start()
    steps = line.steps()
    hops = fsdp_size // 2 - 1
    inserts = {
        0: [lambda: attention(0), lambda: attention(1)],
        hops + 2: [load_out, project],
        2 * hops: [meet_core],
        2 * hops + 2: [meet_x],
    }
    weave(steps, inserts)
    line.finish(local_done=(0,))
    give.wait_recv()
    for copy in (to_core, to_x, give):
        copy.wait_send()


def gather_second(ctx_size, fsdp_size, collective_id, shards, query, key, value, bias, hidden, gain):
    heads, tokens, _ = query.shape
    half, width = hidden.shape
    counts = (fsdp_size // ctx_size, fsdp_size, fsdp_size // ctx_size)
    pieces = (1, 2, 4)
    blocks = []
    for a, shard in enumerate(shards):
        size = shard.shape[0] // pieces[a]
        blocks += [(a, i * size, size) for i in range(pieces[a])]
    outs = [jax.ShapeDtypeStruct((n, *s.shape), s.dtype) for n, s in zip(counts, shards)]
    outs += [
        jax.ShapeDtypeStruct((tokens, heads * 128), LOW),
        jax.ShapeDtypeStruct((heads, tokens, 1), WIDE),
        jax.ShapeDtypeStruct((half, width), WIDE),
        jax.ShapeDtypeStruct((tokens, width), LOW),
    ]
    return pl.pallas_call(
        functools.partial(
            second_kernel, ctx_size, fsdp_size, tuple(blocks), heads, key.shape[0]
        ),
        out_shape=tuple(outs),
        in_specs=[ANY] * 3 + [VMEM] * 6,
        out_specs=(ANY,) * 3 + (VMEM,) * 4,
        scratch_shapes=[
            *LineGather.scratch(fsdp_size, shards, len(blocks)),
            pltpu.VMEM((heads * 128, width), LOW),
            pltpu.VMEM((half, width), WIDE),
            pltpu.VMEM((half, width), LOW),
            pltpu.VMEM((half, width), LOW),
            pltpu.VMEM((half, width), LOW),
            pltpu.VMEM((half, width), LOW),
            DMA((3,)),
            DMA((3,)),
            DMA((heads * HEAD_DIM // min(shards[0].shape[0], HEAD_DIM),)),
        ],
        compiler_params=pltpu.CompilerParams(
            collective_id=collective_id, has_side_effects=True, vmem_limit_bytes=50 * 2**20
        ),
    )(*shards, query, key, value, bias, hidden, gain)


class LineScatter:
    def __init__(self, ctx_size, fsdp_size, kinds, pieces, parts, outs, scratch):
        self.f, self.c, self.z, self.y, self.depth = place(fsdp_size)
        self.n = n = len(parts)
        self.kinds, self.pieces, self.parts, self.outs = kinds, pieces, parts, outs
        self.own, self.beside, self.far = scratch[:n], scratch[n : 2 * n], scratch[2 * n : 3 * n]
        self.cols = [w for w in range(n) if kinds[w] == "cols"]
        count = len(self.cols)
        rest = scratch[3 * n :]
        self.total, self.block, rest = rest[:count], rest[count : 2 * count], rest[2 * count :]
        self.local, self.y_send, self.y_recv, self.z_send, self.z_recv, *more = rest
        if count:
            self.c_send, self.c_recv = more
        self.order = []
        for t in range((self.depth + 1) // 2):
            ends = [self.depth - 1 - t, t]
            self.order += ends if ends[0] != t else [t]
        self.sequence = [(w, t) for w in range(n) for t in self.order]

    @staticmethod
    def shapes(ctx_size, parts, kinds, pieces):
        outs, chunks = [], []
        for part, kind, piece in zip(parts, kinds, pieces):
            if kind == "rows":
                chunks.append(part.shape[1:])
                outs.append(jax.ShapeDtypeStruct(part.shape[1:], WIDE))
                continue
            chunks.append((part.shape[0], *part.shape[2:]))
            rows = part.shape[2]
            for size, flat in piece:
                shape = (rows, ctx_size * size) if flat else (ctx_size, rows, size)
                outs.append(jax.ShapeDtypeStruct(shape, WIDE))
        return outs, chunks

    @staticmethod
    def scratch(fsdp_size, kinds, chunks):
        depth, n = fsdp_size // 2, len(chunks)
        wide = [chunk for chunk, kind in zip(chunks, kinds) if kind == "cols"]
        shapes = [
            *[pltpu.VMEM((depth, *chunk), LOW) for chunk in chunks],
            *[pltpu.VMEM((depth, *chunk), LOW) for chunk in chunks],
            *[pltpu.VMEM((depth + 1, *chunk), LOW) for chunk in chunks],
            *[pltpu.VMEM(chunk, LOW) for chunk in wide],
            *[pltpu.VMEM((3, *chunk[1:]), LOW) for chunk in wide],
            DMA((n, depth)),
            DMA((n, depth)),
            DMA((n, depth)),
            DMA((n, depth)),
            DMA((n, depth + 1)),
        ]
        return shapes + ([DMA((len(wide), 3))] * 2 if wide else [])

    def chunk(self, w, row, column):
        at = row * 2 + column
        return self.parts[w].at[at] if self.kinds[w] == "rows" else self.parts[w].at[:, at]

    def y_copy(self, w, t):
        return remote(
            self.chunk(w, t, 1 - self.y),
            self.beside[w].at[t],
            self.y_send.at[w, t],
            self.y_recv.at[w, t],
            fsdp=self.f ^ 1,
        )

    def z_copy(self, w, t, step, slot):
        return remote(
            self.own[w].at[t],
            self.far[w].at[slot],
            self.z_send.at[w, t],
            self.z_recv.at[w, slot],
            fsdp=(self.z + step) * 2 + self.y,
        )

    def own_copy(self, w, t):
        return pltpu.make_async_copy(self.chunk(w, t, self.y), self.own[w].at[t], self.local.at[w, t])

    def c_copy(self, k, bits):
        return remote(
            self.total[k].at[self.c ^ bits],
            self.block[k].at[bits - 1],
            self.c_send.at[k, bits - 1],
            self.c_recv.at[k, bits - 1],
            ctx=self.c ^ bits,
        )

    def start(self):
        for w, t in self.sequence[:AHEAD]:
            self.y_copy(w, t).start()
        for w, t in self.sequence:
            self.own_copy(w, t).start()

    def step(self, index):
        w, t = self.sequence[index]
        own, beside, far = self.own[w], self.beside[w], self.far[w]
        self.own_copy(w, t).wait()
        self.y_copy(w, t).wait_recv()
        if index + AHEAD < len(self.sequence):
            self.y_copy(*self.sequence[index + AHEAD]).start()
        for step in (1, -1):
            ahead = (t - self.z) * step
            behind = (self.z - step >= 0) & (self.z - step < self.depth)

            @pl.when((ahead > 0) & behind)
            def _():
                self.z_copy(w, t, step, t).wait_recv()
                add_rows(own.at[t], (own.at[t], beside.at[t], far.at[t]))

            @pl.when((ahead > 0) & jnp.logical_not(behind))
            def _():
                add_rows(own.at[t], (own.at[t], beside.at[t]))

            slot = t if step == 1 else t + jnp.where(ahead == 1, self.depth - t, 0)

            @pl.when(ahead > 0)
            def _():
                self.z_copy(w, t, step, slot).start()

    def first_out(self, w):
        return sum(
            1 if self.kinds[v] == "rows" else len(self.pieces[v]) for v in range(w)
        )

    def settle(self, w):
        z, depth = self.z, self.depth
        pl.when(z > 0)(lambda: self.z_copy(w, 0, 1, z).wait_recv())
        pl.when(z < depth - 1)(lambda: self.z_copy(w, 0, 1, depth).wait_recv())
        rows = self.kinds[w] == "rows"
        target = self.outs[self.first_out(w)] if rows else self.total[self.cols.index(w)]
        home = [self.own[w].at[z], self.beside[w].at[z]]
        below, above = self.far[w].at[z], self.far[w].at[depth]
        pl.when(z == 0)(lambda: add_rows(target, (*home, above)))
        pl.when(z == depth - 1)(lambda: add_rows(target, (*home, below)))
        pl.when((z > 0) & (z < depth - 1))(lambda: add_rows(target, (*home, below, above)))
        if not rows:
            for bits in (1, 2, 3):
                self.c_copy(self.cols.index(w), bits).start()

    def spread(self, w):
        k, first = self.cols.index(w), self.first_out(w)
        for bits in (0, 1, 2, 3):
            if bits:
                self.c_copy(k, bits).wait_recv()
            source = self.total[k].at[self.c] if bits == 0 else self.block[k].at[bits - 1]
            at = 0
            for j, (size, flat) in enumerate(self.pieces[w]):
                value = source[:, at : at + size].astype(WIDE)
                if flat:
                    where = pl.ds(pl.multiple_of((self.c ^ bits) * size, 128), size)
                    self.outs[first + j][:, where] = value
                else:
                    self.outs[first + j][self.c ^ bits] = value
                at += size

    def steps(self):
        result = []
        for w in range(self.n):
            for i in range(self.depth):
                result.append(functools.partial(self.step, w * self.depth + i))
            if w:
                result.append(functools.partial(self.settle, w - 1))
        result.append(functools.partial(self.settle, self.n - 1))
        result += [functools.partial(self.spread, w) for w in self.cols]
        return result

    def finish(self):
        for w, t in self.sequence:
            self.y_copy(w, t).wait_send()
            for step in (1, -1):
                pl.when((t - self.z) * step > 0)(
                    lambda w=w, t=t, step=step: self.z_copy(w, t, step, t).wait_send()
                )
        for k in range(len(self.cols)):
            for bits in (1, 2, 3):
                self.c_copy(k, bits).wait_send()


def third_kernel(ctx_size, fsdp_size, kinds, pieces, n_out, heads, kv_heads, *refs):
    n = len(kinds)
    parts, refs = refs[:n], refs[n:]
    far_half, near_half, mid, gain, cot, w_full, refs = *refs[:6], refs[6:]
    query, key, value, bias, log, rows, refs = *refs[:6], refs[6:]
    outs, refs = refs[:n_out], refs[n_out:]
    grad_ffn, grad_mid, mid_low, grad_query, grad_key, grad_value, refs = *refs[:6], refs[6:]
    w_pad, core_in, pair, pair_in, grad_rows, c_send, c_recv, w_sem, *scratch = refs
    c = lax.axis_index("ctx")
    line = LineScatter(ctx_size, fsdp_size, kinds, pieces, parts, outs, scratch)
    tokens, half = query.shape[1], mid.shape[0]
    run_len, tile = half // 2, 128
    scale = HEAD_DIM**-0.5

    def exchange(index, src, dst, bits):
        return remote(src, dst, c_send.at[index], c_recv.at[index], ctx=c ^ bits)

    to_core = exchange(0, far_half, core_in, 1)
    to_x = exchange(1, pair, pair_in, 2)
    give = exchange(2, mid_low.at[pl.ds(0, half)], mid_low.at[pl.ds(half, half)], 1)
    shard = w_full.shape[1]
    piece = min(shard, HEAD_DIM)
    moves = []
    for at in range(0, heads * HEAD_DIM, piece):
        to = at // HEAD_DIM * 128 + at % HEAD_DIM
        src = w_full.at[at // shard, pl.ds(at % shard, piece)]
        moves.append(pltpu.make_async_copy(src, w_pad.at[pl.ds(to, piece)], w_sem.at[len(moves)]))

    def load_out():
        for move in moves:
            move.start()
        for h in range(heads):
            w_pad[pl.ds(h * 128 + HEAD_DIM, 128 - HEAD_DIM)] = jnp.zeros(
                (128 - HEAD_DIM, w_pad.shape[1]), LOW
            )

    def meet_core():
        to_core.wait_recv()
        add_rows(pair, (near_half, core_in))
        to_x.start()

    def meet_x():
        to_x.wait_recv()
        for block in (0, 1):

            def body(at, block=block):
                here = pl.ds(pl.multiple_of(at.start + block * run_len, 16), 16)
                there = pl.ds(pl.multiple_of(at.start + (1 - block) * run_len, 16), 16)
                grad = pair[here].astype(WIDE) + pair_in[there].astype(WIDE)
                grad_ffn[here] = grad
                recip = inverse_rms(mid[here])
                scaled = mid[here] * recip
                total = cot[here].astype(WIDE) + norm_backward(grad, scaled, recip, gain[0:1])
                grad_mid[here] = total
                mid_low[here] = total.astype(LOW)

            row_loop(run_len, body)
        give.start()

    def attend_back():
        for move in moves:
            move.wait()
        give.wait_recv()

        def back_out(at):
            grad_rows[at] = lax.dot_general(
                mid_low[at], w_pad[...], (((1,), (1,)), ((), ())), preferred_element_type=WIDE
            ).astype(LOW)

        row_loop(tokens, back_out, tile)
        grad_key[...] = jnp.zeros_like(grad_key)
        grad_value[...] = jnp.zeros_like(grad_value)

        def body(i, carry):
            h = i // (tokens // tile)
            r = i % (tokens // tile)
            at = pl.ds(pl.multiple_of(r * tile, tile), tile)
            lanes = pl.ds(pl.multiple_of(h * 128, 128), 128)
            g = h // (heads // kv_heads)
            q = query[h, at]
            s = lax.dot_general(
                q, key[g], (((1,), (1,)), ((), ())), preferred_element_type=WIDE
            )
            p = jnp.exp(s * scale + bias[at] - log[h, at])
            grad_out = grad_rows[at, lanes]
            delta = jnp.sum(
                grad_out.astype(WIDE) * rows[at, lanes].astype(WIDE), axis=-1, keepdims=True
            )
            grad_p = lax.dot_general(
                grad_out, value[g], (((1,), (1,)), ((), ())), preferred_element_type=WIDE
            )
            grad_s = (p * (grad_p - delta)).astype(LOW)
            grad_query[h, at] = jnp.dot(grad_s, key[g], preferred_element_type=WIDE) * scale
            grad_key[g] = grad_key[g] + contract_rows(grad_s, q)
            grad_value[g] = grad_value[g] + contract_rows(p.astype(LOW), grad_out)
            return carry

        lax.fori_loop(0, heads * (tokens // tile), body, 0)
        grad_key[...] = grad_key[...] * scale

    greet(fsdp_size)
    to_core.start()
    line.start()
    inserts = {
        0: [load_out, meet_core],
        1: [meet_x],
        2: [attend_back],
    }
    weave(line.steps(), inserts)
    line.finish()
    for copy in (to_core, to_x, give):
        copy.wait_send()


def scatter_third(ctx_size, fsdp_size, collective_id, parts, kinds, pieces, small):
    outs, chunks = LineScatter.shapes(ctx_size, parts, kinds, pieces)
    n_out = len(outs)
    far_half, near_half, mid, gain, cot, w_full, query, key = small[:8]
    half, width = mid.shape
    heads, tokens, _ = query.shape
    kv_heads = key.shape[0]
    outs += [
        jax.ShapeDtypeStruct((half, width), WIDE),
        jax.ShapeDtypeStruct((half, width), WIDE),
        jax.ShapeDtypeStruct((tokens, width), LOW),
        jax.ShapeDtypeStruct(query.shape, WIDE),
        jax.ShapeDtypeStruct(key.shape, WIDE),
        jax.ShapeDtypeStruct(key.shape, WIDE),
    ]
    results = pl.pallas_call(
        functools.partial(
            third_kernel, ctx_size, fsdp_size, kinds, pieces, n_out, heads, kv_heads
        ),
        out_shape=tuple(outs),
        in_specs=[ANY] * len(parts) + [VMEM] * 5 + [ANY] + [VMEM] * 6,
        out_specs=(VMEM,) * len(outs),
        scratch_shapes=[
            pltpu.VMEM((heads * 128, width), LOW),
            pltpu.VMEM((half, width), LOW),
            pltpu.VMEM((half, width), LOW),
            pltpu.VMEM((half, width), LOW),
            pltpu.VMEM((tokens, heads * 128), LOW),
            DMA((3,)),
            DMA((3,)),
            DMA((heads * HEAD_DIM // min(w_full.shape[1], HEAD_DIM),)),
            *LineScatter.scratch(fsdp_size, kinds, chunks),
        ],
        compiler_params=pltpu.CompilerParams(
            collective_id=collective_id, has_side_effects=True, vmem_limit_bytes=58 * 2**20
        ),
    )(*parts, *small)
    return results[:n_out], results[n_out:]


def last_kernel(ctx_size, fsdp_size, kinds, pieces, n_out, *refs):
    n = len(kinds)
    parts, refs = refs[:n], refs[n:]
    out_far, out_near, in_far, in_near, mid, grad_mid, hidden, gain, grad_ffn, refs = (
        *refs[:9],
        refs[9:],
    )
    outs, refs = refs[:n_out], refs[n_out:]
    output, grad_in, gain_out, refs = *refs[:3], refs[3:]
    core_in, swap_out, swap_in, gain_own, gain_in, c_send, c_recv, g_send, g_recv, *scratch = refs
    line = LineScatter(ctx_size, fsdp_size, kinds, pieces, parts, outs, scratch)
    f, c, z, y, depth = place(fsdp_size)
    half = out_near.shape[0]
    run_len = half // 2

    def exchange(index, src, dst, bits):
        return remote(src, dst, c_send.at[index], c_recv.at[index], ctx=c ^ bits)

    cores = [exchange(0, in_far, core_in.at[0], 1), exchange(1, out_far, core_in.at[1], 1)]
    swaps = [exchange(2 + i, swap_out.at[i], swap_in.at[i], 2) for i in (0, 1)]
    near = (in_near, out_near)

    def meet_core(i):
        cores[i].wait_recv()

        def body(at):
            there = pl.ds(pl.multiple_of(at.start + run_len, 16), 16)
            swap_out[i, at] = (near[i][there] + core_in[i, there].astype(WIDE)).astype(LOW)

        row_loop(run_len, body)
        swaps[i].start()

    def own_sum(i, at):
        return near[i][at] + core_in[i, at].astype(WIDE) + swap_in[i, at].astype(WIDE)

    def meet_in():
        swaps[0].wait_recv()
        gain_own[...] = jnp.zeros_like(gain_own)

        def body(at):
            grad = own_sum(0, at)
            values = hidden[at].astype(WIDE)
            recip = inverse_rms(values)
            scaled = values * recip
            grad_in[at] = grad_mid[at] + norm_backward(grad, scaled, recip, gain[0:1])
            gain_own[0, 0:1] = gain_own[0, 0:1] + jnp.sum(grad * scaled, axis=0, keepdims=True)
            mids = mid[at]
            gain_own[0, 1:2] = gain_own[0, 1:2] + jnp.sum(
                grad_ffn[at] * (mids * inverse_rms(mids)), axis=0, keepdims=True
            )

        row_loop(run_len, body)

    def meet_out():
        swaps[1].wait_recv()

        def body(at):
            output[at] = (mid[at] + own_sum(1, at)).astype(LOW)

        row_loop(run_len, body)

    def gain_copy(i):
        where = ({"ctx": c ^ 1}, {"ctx": c ^ 2}, {"fsdp": f ^ 1})[i]
        return remote(gain_own.at[i], gain_in.at[i], g_send.at[i], g_recv.at[i], **where)

    def gain_meet(i):
        if i:
            gain_copy(i - 1).wait_recv()
            gain_own[i] = gain_own[i - 1] + gain_in[i - 1]
        gain_copy(i).start()

    gain_far = 3

    def up_copy():
        return remote(
            gain_own.at[4], gain_in.at[gain_far], g_send.at[3], g_recv.at[3], fsdp=(z + 1) * 2 + y
        )

    def down_copy():
        return remote(
            gain_own.at[5],
            gain_in.at[gain_far + 1],
            g_send.at[4],
            g_recv.at[4],
            fsdp=(z - 1) * 2 + y,
        )

    def gain_line():
        gain_copy(2).wait_recv()
        gain_own[3] = gain_own[2] + gain_in[2]

        @pl.when(z > 0)
        def _():
            remote(
                gain_own.at[4], gain_in.at[gain_far], g_send.at[3], g_recv.at[3], ctx=c ^ 1
            ).wait_recv()
            gain_own[4] = gain_own[3] + gain_in[gain_far]

        @pl.when(z == 0)
        def _():
            gain_own[4] = gain_own[3]

        pl.when(z + 1 < depth)(lambda: up_copy().start())

        @pl.when(z + 1 < depth)
        def _():
            remote(
                gain_own.at[5], gain_in.at[gain_far + 1], g_send.at[4], g_recv.at[4], ctx=c ^ 1
            ).wait_recv()
            gain_own[5] = gain_own[3] + gain_in[gain_far + 1]

        @pl.when(z + 1 == depth)
        def _():
            gain_own[5] = gain_own[3]

        pl.when(z > 0)(lambda: down_copy().start())
        gain_out[...] = gain_own[4] + gain_own[5] - gain_own[3]

    greet(fsdp_size)
    for copy in cores:
        copy.start()
    line.start()
    steps = line.steps()
    inserts = {
        0: [lambda: meet_core(0), lambda: meet_core(1)],
        2: [meet_in, lambda: gain_meet(0)],
        3: [lambda: gain_meet(1), meet_out],
        4: [lambda: gain_meet(2)],
        5: [gain_line],
    }
    weave(steps, inserts)
    line.finish()
    for copy in (*cores, *swaps, gain_copy(0), gain_copy(1), gain_copy(2)):
        copy.wait_send()
    pl.when(z + 1 < depth)(lambda: up_copy().wait_send())
    pl.when(z > 0)(lambda: down_copy().wait_send())


def scatter_last(ctx_size, fsdp_size, collective_id, parts, kinds, pieces, small):
    outs, chunks = LineScatter.shapes(ctx_size, parts, kinds, pieces)
    n_out = len(outs)
    half, width = small[0].shape
    run_len = half // 2
    outs += [
        jax.ShapeDtypeStruct((run_len, width), LOW),
        jax.ShapeDtypeStruct((run_len, width), WIDE),
        jax.ShapeDtypeStruct((8, width), WIDE),
    ]
    results = pl.pallas_call(
        functools.partial(last_kernel, ctx_size, fsdp_size, kinds, pieces, n_out),
        out_shape=tuple(outs),
        in_specs=[ANY] * len(parts) + [VMEM] * 9,
        out_specs=(VMEM,) * len(outs),
        scratch_shapes=[
            pltpu.VMEM((2, half, width), LOW),
            pltpu.VMEM((2, run_len, width), LOW),
            pltpu.VMEM((2, run_len, width), LOW),
            pltpu.VMEM((6, 8, width), WIDE),
            pltpu.VMEM((5, 8, width), WIDE),
            DMA((4,)),
            DMA((4,)),
            DMA((5,)),
            DMA((5,)),
            *LineScatter.scratch(fsdp_size, kinds, chunks),
        ],
        compiler_params=pltpu.CompilerParams(
            collective_id=collective_id, has_side_effects=True, vmem_limit_bytes=50 * 2**20
        ),
    )(*parts, *small)
    return results[:n_out], results[n_out:]


def inverse_rms(values):
    return lax.rsqrt(jnp.mean(values * values, axis=-1, keepdims=True) + EPS)


def norm_backward(grad_normed, scaled, inv_rms, gain):
    grad_scaled = grad_normed * gain
    return inv_rms * (
        grad_scaled - scaled * jnp.mean(grad_scaled * scaled, axis=-1, keepdims=True)
    )


def rope_tables(positions):
    half_dim = HEAD_DIM // 2
    freq_index = jnp.arange(half_dim, dtype=jnp.float32)
    frequency = jnp.exp(freq_index * (-2.0 / HEAD_DIM) * math.log(ROPE_BASE))
    angles = positions.astype(jnp.float32)[:, None] * frequency
    return (jnp.cos(angles)[:, None, :], jnp.sin(angles)[:, None, :])


def rotate(tensor, cosine, sine):
    half_dim = tensor.shape[-1] // 2
    front, back = tensor[..., :half_dim], tensor[..., half_dim:]
    return jnp.concatenate([front * cosine - back * sine, back * cosine + front * sine], axis=-1)


def rotate_back(tensor, cosine, sine):
    return rotate(tensor, cosine, -sine)


def dot(left, right):
    return jnp.dot(left, right, preferred_element_type=jnp.float32)


def contract_rows(left, right):
    return lax.dot_general(
        left, right, (((0,), (0,)), ((), ())), preferred_element_type=jnp.float32
    )


def times_transpose(left, weight):
    return lax.dot_general(
        left, weight, (((1,), (1,)), ((), ())), preferred_element_type=jnp.float32
    )


def make_step(ctx_size, fsdp_size):
    def per_device(
        hidden_in,
        segments,
        w_query,
        w_key,
        w_value,
        w_out,
        w_gate,
        w_up,
        w_down,
        attn_gain,
        ffn_gain,
        grad_out,
    ):
        _, run_len, width = hidden_in.shape
        c_index, f_index = lax.axis_index("ctx"), lax.axis_index("fsdp")
        heads, kv_heads = HEADS // ctx_size, KV_HEADS // ctx_size
        q_cols, kv_cols = heads * HEAD_DIM, kv_heads * HEAD_DIM
        ff = w_gate.shape[1] // ctx_size
        shard = width // fsdp_size
        owned = shard // ctx_size
        half = 2 * run_len

        def columns(weight, size):
            return lax.dynamic_slice_in_dim(weight, c_index * size, size, 1)

        own_hidden = hidden_in.reshape(run_len, width)
        blocks, (hidden, cotangent, seg_rows) = gather_first(
            ctx_size,
            fsdp_size,
            0,
            (
                jnp.concatenate(
                    [columns(w_query, q_cols), columns(w_key, kv_cols), columns(w_value, kv_cols)],
                    axis=1,
                ),
                jnp.pad(jnp.stack([attn_gain, ffn_gain]), ((0, 6), (0, -shard % 128))),
            ),
            (own_hidden, grad_out.reshape(run_len, width), jnp.broadcast_to(segments, (8, run_len))),
        )
        full_qkv = blocks[0].reshape(width, q_cols + 2 * kv_cols)
        gains = jnp.swapaxes(blocks[1][:, :2, :shard], 0, 1).reshape(2, width).astype(WIDE)
        attn_gain_rows = jnp.broadcast_to(gains[:1], (8, width))
        ffn_gain_rows = jnp.broadcast_to(gains[1:], (8, width))
        hidden = hidden.reshape(-1, width)
        cotangent = cotangent.reshape(-1, width)

        seg_flat = seg_rows[:, 0].reshape(-1)
        runs = jnp.stack([c_index, c_index ^ 2, c_index ^ 1, c_index ^ 3])
        ids = (runs[:, None] * run_len + jnp.arange(run_len, dtype=jnp.int32)).reshape(-1)
        before = jnp.sum((seg_flat[None, :] < seg_flat[:, None]).astype(jnp.int32), axis=-1)
        cosine, sine = rope_tables(ids - before)
        allowed = (seg_flat[None, :] == seg_flat[:, None]) & (ids[None, :] <= ids[:, None])
        bias = jnp.where(allowed, 0.0, -1e30).astype(WIDE)
        tokens = ids.shape[0]

        def to_heads(tensor):
            padded = jnp.pad(tensor.astype(LOW), ((0, 0), (0, 0), (0, 128 - HEAD_DIM)))
            return jnp.swapaxes(padded, 0, 1)

        def from_heads(tensor):
            return jnp.swapaxes(tensor[:, :, :HEAD_DIM], 0, 1)

        hidden_wide = hidden.astype(WIDE)
        attn_normed = (hidden_wide * inverse_rms(hidden_wide) * gains[0]).astype(LOW)
        projected = dot(attn_normed, full_qkv)
        query = projected[:, :q_cols].reshape(tokens, heads, HEAD_DIM)
        key = projected[:, q_cols : q_cols + kv_cols].reshape(tokens, kv_heads, HEAD_DIM)
        value = projected[:, q_cols + kv_cols :].reshape(tokens, kv_heads, HEAD_DIM)
        query = to_heads(rotate(query, cosine, sine))
        key = to_heads(rotate(key, cosine, sine))
        value = to_heads(value)

        gate_up_shard = jnp.concatenate([columns(w_gate, ff), columns(w_up, ff)], axis=1)
        full_out, full_gate_up, full_down, attn_rows, log_total, mid, ffn_normed = gather_second(
            ctx_size,
            fsdp_size,
            1,
            (w_out, gate_up_shard, w_down),
            query,
            key,
            value,
            bias,
            hidden[:half],
            ffn_gain_rows,
        )
        full_gate_up = full_gate_up.reshape(width, 2 * ff)
        full_down = full_down.reshape(ff, width)

        gate_up = dot(ffn_normed, full_gate_up)
        gate, up = gate_up[:, :ff], gate_up[:, ff:]
        sigmoid = jax.nn.sigmoid(gate)
        silu = gate * sigmoid
        inner = (silu * up).astype(LOW)
        part_output = dot(inner, full_down)
        part_down = contract_rows(inner, cotangent).astype(LOW)
        grad_inner = times_transpose(cotangent, full_down)
        grad_gate = grad_inner * up * sigmoid * (1.0 + gate * (1.0 - sigmoid))
        grad_gate_up = jnp.concatenate(
            [grad_gate.astype(LOW), (grad_inner * silu).astype(LOW)], axis=1
        )
        part_ffn = times_transpose(grad_gate_up, full_gate_up)
        part_gate_up = contract_rows(ffn_normed, grad_gate_up).astype(LOW)

        (grad_gate_w, grad_up_w, grad_down_w), back = scatter_third(
            ctx_size,
            fsdp_size,
            2,
            (
                part_gate_up.reshape(ctx_size, fsdp_size, owned, 2 * ff),
                part_down.reshape(fsdp_size, -1, width),
            ),
            ("cols", "rows"),
            (((ff, True), (ff, True)), None),
            (
                part_ffn[half:].astype(LOW),
                part_ffn[:half],
                mid,
                ffn_gain_rows,
                cotangent[:half],
                full_out,
                query,
                key,
                value,
                bias,
                log_total,
                attn_rows,
            ),
        )
        grad_ffn, grad_mid, grad_mid_low, grad_query, grad_key, grad_value = back

        grad_qkv = jnp.concatenate(
            [
                rotate_back(from_heads(grad_query), cosine, sine).astype(LOW).reshape(tokens, -1),
                rotate_back(from_heads(grad_key), cosine, sine).astype(LOW).reshape(tokens, -1),
                from_heads(grad_value).astype(LOW).reshape(tokens, -1),
            ],
            axis=1,
        )
        part_qkv = contract_rows(attn_normed, grad_qkv).astype(LOW)
        part_out = contract_rows(attn_rows, grad_mid_low).astype(LOW)
        part_out = part_out.reshape(heads, 128, width)[:, :HEAD_DIM]
        part_in = times_transpose(grad_qkv, full_qkv)

        (grad_query_w, grad_kv_w, grad_out_w), (output, grad_in, gain_sums) = scatter_last(
            ctx_size,
            fsdp_size,
            3,
            (
                part_qkv.reshape(ctx_size, fsdp_size, owned, -1),
                part_out.reshape(fsdp_size, -1, width),
            ),
            ("cols", "rows"),
            (((q_cols, True), (2 * kv_cols, False)), None),
            (
                part_output[half:].astype(LOW),
                part_output[:half],
                part_in[half:].astype(LOW),
                part_in[:half],
                mid,
                grad_mid,
                own_hidden,
                attn_gain_rows,
                grad_ffn,
            ),
        )
        grad_kv_w = jnp.swapaxes(grad_kv_w, 0, 1)
        gain_own = lax.dynamic_slice_in_dim(
            gain_sums[:2], (c_index * fsdp_size + f_index) * owned, owned, 1
        )

        return (
            output[None],
            grad_in[None],
            grad_query_w,
            grad_kv_w[:, :, :kv_cols].reshape(owned, -1),
            grad_kv_w[:, :, kv_cols:].reshape(owned, -1),
            grad_out_w,
            grad_gate_w,
            grad_up_w,
            grad_down_w,
            gain_own[0],
            gain_own[1],
        )

    return per_device


def solution(mesh):
    rows = P("fsdp", None)
    spread = P(("ctx", "fsdp"), None)
    runs = P("fsdp", "ctx", None)
    return jax.shard_map(
        make_step(mesh.shape["ctx"], mesh.shape["fsdp"]),
        mesh=mesh,
        in_specs=(runs, P("fsdp", "ctx"), *[rows] * 7, P("fsdp"), P("fsdp"), runs),
        out_specs=(runs, runs, *[spread] * 7, P(("ctx", "fsdp")), P(("ctx", "fsdp"))),
        check_vma=False,
    )
```

```python
import functools
import math

import jax
import jax.numpy as jnp
from jax import lax
from jax.experimental import pallas as pl
from jax.experimental.pallas import tpu as pltpu
from jax.sharding import PartitionSpec as P

HEADS = 16
KV_HEADS = 8
HEAD_DIM = 96
EPS = 1e-05
ROPE_BASE = 100000.0

AHEAD = 4
MESH = pl.DeviceIdType.MESH
ANY = pl.BlockSpec(memory_space=pl.ANY)
VMEM = pl.BlockSpec(memory_space=pltpu.VMEM)
DMA = pltpu.SemaphoreType.DMA
LOW = jnp.bfloat16
WIDE = jnp.float32


def remote(src, dst, send, recv, **where):
    return pltpu.make_async_remote_copy(
        src_ref=src,
        dst_ref=dst,
        send_sem=send,
        recv_sem=recv,
        device_id=where,
        device_id_type=MESH,
    )


def place(fsdp_size):
    f, c = lax.axis_index("fsdp"), lax.axis_index("ctx")
    return f, c, f // 2, f % 2, fsdp_size // 2


def greet(fsdp_size, all_rows=False):
    f, c, z, y, depth = place(fsdp_size)
    barrier = pltpu.get_barrier_semaphore()
    for bits in (1, 2, 3):
        pl.semaphore_signal(barrier, inc=1, device_id={"ctx": c ^ bits}, device_id_type=MESH)
    pl.semaphore_signal(barrier, inc=1, device_id={"fsdp": f ^ 1}, device_id_type=MESH)
    if all_rows:
        for shift in range(1, depth):
            row = (z + shift) % depth
            pl.semaphore_signal(
                barrier, inc=1, device_id={"fsdp": row * 2 + y}, device_id_type=MESH
            )
        pl.semaphore_wait(barrier, depth + 3)
        return
    for step in (1, -1):
        near = z + step

        @pl.when((near >= 0) & (near < depth))
        def _():
            pl.semaphore_signal(
                barrier, inc=1, device_id={"fsdp": near * 2 + y}, device_id_type=MESH
            )

    pl.semaphore_wait(barrier, 4 + jnp.minimum(z, 1) + jnp.minimum(depth - 1 - z, 1))


class LineGather:
    def __init__(self, ctx_size, fsdp_size, masked, blocks, owns, fulls, stages, sems):
        self.sizes = ctx_size, fsdp_size
        self.f, self.c, self.z, self.y, self.depth = place(fsdp_size)
        self.masked, self.blocks = masked, blocks
        self.owns, self.fulls, self.stages = owns, fulls, stages
        self.z_send, self.z_recv, self.y_send, self.y_recv, self.local = sems
        self.beside_done = set()

    @staticmethod
    def scratch(fsdp_size, arrays, count):
        depth = fsdp_size // 2
        return [
            *[pltpu.VMEM(a.shape, a.dtype) for a in arrays],
            DMA((count, 2, depth - 1)),
            DMA((count, 2, depth - 1)),
            DMA((count, 2 * depth - 1)),
            DMA((count, 2 * depth - 1)),
            DMA((len(arrays),)),
        ]

    def held(self, a, row):
        there = (row >= 0) & (row < self.depth)
        if self.masked[a]:
            span = self.depth // self.sizes[0]
            there = there & (row >= self.c * span) & (row < (self.c + 1) * span)
        return there

    def entry(self, a, row, column):
        base = self.c * (self.sizes[1] // self.sizes[0]) if self.masked[a] else 0
        return row * 2 + column - base

    def spot(self, b, row, column):
        a, low, size = self.blocks[b]
        return self.fulls[a].at[self.entry(a, row, column), pl.ds(low, size)]

    def source(self, b, row):
        a, low, size = self.blocks[b]
        return self.owns[a].at[pl.ds(low, size)] if row is None else self.spot(b, row, self.y)

    def z_copy(self, b, way, hop):
        step = 1 if way == 0 else -1
        row = self.z - step * (hop - 1)
        near = self.z + step
        copy = remote(
            self.source(b, None if hop == 1 else row),
            self.spot(b, row, self.y),
            self.z_send.at[b, way, hop - 1],
            self.z_recv.at[b, way, hop - 1],
            fsdp=near * 2 + self.y,
        )
        return copy, self.held(self.blocks[b][0], row) & (near >= 0) & (near < self.depth)

    def row_of(self, slot):
        return self.z - slot if slot < self.depth else self.z + (slot - self.depth + 1)

    def y_copy(self, b, slot):
        row = self.row_of(slot)
        copy = remote(
            self.source(b, row if slot else None),
            self.spot(b, row, self.y),
            self.y_send.at[b, slot],
            self.y_recv.at[b, slot],
            fsdp=self.f ^ 1,
        )
        return copy, self.held(self.blocks[b][0], row)

    @staticmethod
    def begin(pair):
        pl.when(pair[1])(lambda: pair[0].start())

    def send_own(self, b):
        self.begin(self.z_copy(b, 0, 1))
        self.begin(self.z_copy(b, 1, 1))
        self.begin(self.y_copy(b, 0))

    def local_in(self, a):
        return pltpu.make_async_copy(self.owns[a], self.stages[a], self.local.at[a])

    def local_out(self, a):
        spot = self.fulls[a].at[self.entry(a, self.z, self.y)]
        return pltpu.make_async_copy(self.stages[a], spot, self.local.at[a])

    def start(self):
        for a in range(len(self.owns)):
            self.local_in(a).start()
        for b in range(min(2, len(self.blocks))):
            self.send_own(b)
        for a in range(len(self.owns)):
            self.local_in(a).wait()
            pl.when(self.held(a, self.z))(lambda a=a: self.local_out(a).start())

    def step(self, b, hop):
        a = self.blocks[b][0]
        for way in (0, 1):
            row = self.z - hop if way == 0 else self.z + hop

            @pl.when(self.held(a, row))
            def _():
                remote(
                    self.source(b, None),
                    self.spot(b, row, self.y),
                    self.z_send.at[b, way, hop - 1],
                    self.z_recv.at[b, way, hop - 1],
                    fsdp=self.f ^ 1,
                ).wait_recv()

            if hop + 1 < self.depth:
                self.begin(self.z_copy(b, way, hop + 1))
            self.begin(self.y_copy(b, hop if way == 0 else self.depth - 1 + hop))
        if hop == 1 and b + 2 < len(self.blocks):
            self.send_own(b + 2)

    def steps(self):
        return [
            ((b, hop), functools.partial(self.step, b, hop))
            for b in range(len(self.blocks))
            for hop in range(1, self.depth)
        ]

    def wait_local(self, a):
        pl.when(self.held(a, self.z))(lambda: self.local_out(a).wait())

    def wait_beside(self, b):
        if b in self.beside_done:
            return
        self.beside_done.add(b)
        for slot in range(2 * self.depth - 1):
            row = self.row_of(slot)

            @pl.when(self.held(self.blocks[b][0], row))
            def _():
                remote(
                    self.source(b, None),
                    self.spot(b, row, 1 - self.y),
                    self.y_send.at[b, slot],
                    self.y_recv.at[b, slot],
                    fsdp=self.f ^ 1,
                ).wait_recv()

    def finish(self, local_done=()):
        for b in range(len(self.blocks)):
            self.wait_beside(b)
        pairs = []
        for b in range(len(self.blocks)):
            for hop in range(1, self.depth):
                pairs += [self.z_copy(b, 0, hop), self.z_copy(b, 1, hop)]
            pairs += [self.y_copy(b, slot) for slot in range(2 * self.depth - 1)]
        for copy, there in pairs:
            pl.when(there)(lambda copy=copy: copy.wait_send())
        for a in range(len(self.owns)):
            if a not in local_done:
                self.wait_local(a)


def weave(steps, inserts):
    for name, step in steps:
        for extra in inserts.pop(name, ()):
            extra()
        step()
    assert not inserts


def row_loop(total, body, rows=16):
    rows = rows if total % rows == 0 else total

    def run(step, carry):
        body(pl.ds(pl.multiple_of(step * rows, rows), rows))
        return carry

    lax.fori_loop(0, total // rows, run, 0)


def add_rows(out_ref, terms):
    shape = out_ref.shape
    leads = [None] if len(shape) == 2 else list(range(shape[0]))

    def body(at):
        for lead in leads:
            index = (at,) if lead is None else (lead, at)
            value = None
            for ref in terms:
                part = ref[index].astype(WIDE)
                value = part if value is None else value + part
            out_ref[index] = value.astype(out_ref.dtype)

    row_loop(shape[-2], body)


def front_kernel(ctx_size, fsdp_size, blocks, heads, kv_heads, *refs):
    owns, runs, frequency, refs = refs[:5], refs[5:9], refs[9], refs[10:]
    fulls, alls, refs = [None, *refs[:4]], refs[4:6], refs[6:]
    query, key, value, bias, cosine, sine, refs = *refs[:6], refs[6:]
    attn_normed, gains, rows_out, log_out, mid_out, normed, refs = *refs[:6], refs[6:]
    stages, sems, refs = refs[:5], refs[5:10], refs[10:]
    fulls[0], seg_rows, seg_cols, stage_runs, refs = refs[0], refs[1], refs[2], refs[3:5], refs[5:]
    select, w_proj, w_pad, kept, core_out, core_in, pair, pair_in, refs = *refs[:8], refs[8:]
    c_send, c_recv, r_send, r_recv, local, w_sem = refs
    c = lax.axis_index("ctx")
    masked = (False, False, True, False, True)
    line = LineGather(ctx_size, fsdp_size, masked, blocks, owns, fulls, stages, sems)
    hidden_all, cot_all = alls
    tokens = query.shape[1]
    run_len = tokens // ctx_size
    half = 2 * run_len
    scale = HEAD_DIM**-0.5
    tile = 128
    assert run_len == tile
    relation = (0, 2, 1, 3)

    targets = (seg_rows, seg_cols, hidden_all, cot_all)
    sources = (runs[2], runs[3], runs[0], runs[1])

    def run_copy(r, bits):
        return remote(
            sources[r],
            targets[r].at[relation[bits]],
            r_send.at[r, bits - 1],
            r_recv.at[r, bits - 1],
            ctx=c ^ bits,
        )

    def run_in(r):
        dst = targets[r].at[0] if r < 3 else stage_runs[0]
        return pltpu.make_async_copy(sources[r], dst, local.at[r])

    def run_out():
        return pltpu.make_async_copy(stage_runs[0], cot_all.at[0], local.at[3])

    def start_runs():
        for r in (0, 1, 2, 3):
            run_in(r).start()
        for r in (0, 1, 2):
            for bits in (2, 1, 3):
                run_copy(r, bits).start()
        run_in(3).wait()
        run_out().start()

    def tables():
        for r in (0, 1, 2):
            run_in(r).wait()
            for bits in (2, 1, 3):
                run_copy(r, bits).wait_recv()
        for bits in (2, 1, 3):
            run_copy(3, bits).start()
        down = lax.broadcasted_iota(jnp.int32, (tile, tile), 0)
        across = lax.broadcasted_iota(jnp.int32, (tile, tile), 1)
        for r in range(ctx_size):
            at = pl.ds(r * tile, tile)
            own_seg = seg_cols[r]
            ids = (c ^ relation[r]) * tile + down
            before = jnp.zeros((tile, 1), WIDE)
            for k in range(ctx_size):
                other = seg_rows[k, 0:1]
                smaller = jnp.where(other < own_seg, 1.0, 0.0)
                before = before + jnp.sum(smaller, axis=-1, keepdims=True)
                seen = (other == own_seg) & ((c ^ relation[k]) * tile + across <= ids)
                bias[at, k * tile : (k + 1) * tile] = jnp.where(seen, 0.0, -1e30).astype(LOW)
            angles = (ids.astype(WIDE) - before) * frequency[0:1]
            cosine[at] = jnp.cos(angles)
            sine[at] = jnp.sin(angles)

    def first_norm():
        line.wait_beside(0)
        line.wait_local(0)
        shard = owns[1].shape[0]
        lanes = fulls[0].shape[-1]
        width = gains.shape[1]
        total = None
        for f in range(fsdp_size):
            wide = jnp.concatenate(
                [fulls[0][f], jnp.zeros((8, width - lanes), WIDE)], axis=1
            )
            wide = pltpu.roll(wide, f * shard, 1) if f else wide
            total = wide if total is None else total + wide
        gains[...] = total
        for r in range(ctx_size):

            def body(at, r=r):
                values = hidden_all[r, at].astype(WIDE)
                there = pl.ds(pl.multiple_of(at.start + r * run_len, 16), 16)
                attn_normed[there] = (values * inverse_rms(values) * gains[0:1]).astype(LOW)

            row_loop(run_len, body)

    def spread_weights():
        line.wait_beside(1)
        line.wait_local(1)
        shard = owns[1].shape[0]
        for f in range(fsdp_size):
            w_proj[f * shard : (f + 1) * shard] = jnp.dot(
                fulls[1][f], select[...], preferred_element_type=WIDE
            ).astype(LOW)

    def project_in():
        def body(at):
            for h in range(heads + 2 * kv_heads):
                lanes = pl.ds(h * 128, 128)
                tensor = jnp.dot(
                    attn_normed[at], w_proj[:, lanes], preferred_element_type=WIDE
                )
                if h < heads + kv_heads:
                    tensor = turn(tensor, cosine[at], sine[at])
                ref, g = (
                    (query, h)
                    if h < heads
                    else (key, h - heads)
                    if h < heads + kv_heads
                    else (value, h - heads - kv_heads)
                )
                ref[g, at] = tensor.astype(LOW)

        row_loop(tokens, body, tile)

    def attention(part):
        def body(i, carry):
            h = i // (tokens // tile)
            r = i % (tokens // tile)
            at = pl.ds(pl.multiple_of(r * tile, tile), tile)
            g = h // (heads // kv_heads)
            s = lax.dot_general(
                query[h, at], key[g], (((1,), (1,)), ((), ())), preferred_element_type=WIDE
            )
            s = s * scale + bias[at].astype(WIDE)
            top = jnp.max(s, axis=-1, keepdims=True)
            log = top + jnp.log(jnp.sum(jnp.exp(s - top), axis=-1, keepdims=True))
            p = jnp.exp(s - log).astype(LOW)
            mixed = jnp.dot(p, value[g], preferred_element_type=WIDE)
            rows_out[at, pl.ds(pl.multiple_of(h * 128, 128), 128)] = mixed.astype(LOW)
            log_out[h, at] = log
            return carry

        count = heads * (tokens // tile)
        lax.fori_loop(part * count // 2, (part + 1) * count // 2, body, 0)

    def exchange(index, src, dst, bits):
        return remote(src, dst, c_send.at[index], c_recv.at[index], ctx=c ^ bits)

    to_core = exchange(0, core_out, core_in, 1)
    to_x = exchange(1, pair, pair_in, 2)
    give = exchange(2, normed.at[pl.ds(0, half)], normed.at[pl.ds(half, half)], 1)

    shard = owns[2].shape[0]
    piece = min(shard, HEAD_DIM)
    moves = []
    for at in range(0, heads * HEAD_DIM, piece):
        to = at // HEAD_DIM * 128 + at % HEAD_DIM
        src = fulls[2].at[at // shard, pl.ds(at % shard, piece)]
        moves.append(pltpu.make_async_copy(src, w_pad.at[pl.ds(to, piece)], w_sem.at[len(moves)]))

    def load_out():
        line.wait_beside(2)
        line.wait_local(2)
        for move in moves:
            move.start()
        for h in range(heads):
            w_pad[pl.ds(h * 128 + HEAD_DIM, 128 - HEAD_DIM)] = jnp.zeros(
                (128 - HEAD_DIM, w_pad.shape[1]), LOW
            )
        for move in moves:
            move.wait()

    def project():
        def far(at):
            value_rows = rows_out[pl.ds(pl.multiple_of(at.start + half, tile), tile)]
            core_out[at] = jnp.dot(value_rows, w_pad[...], preferred_element_type=WIDE).astype(LOW)

        row_loop(half, far, tile)
        to_core.start()

        def near(at):
            kept[at] = jnp.dot(rows_out[at], w_pad[...], preferred_element_type=WIDE)

        row_loop(half, near, tile)

    def meet_core():
        to_core.wait_recv()
        add_rows(pair, (kept, core_in))
        to_x.start()

    def meet_x():
        to_x.wait_recv()
        for block in (0, 1):

            def body(at, block=block):
                here = pl.ds(pl.multiple_of(at.start + block * run_len, 16), 16)
                there = pl.ds(pl.multiple_of(at.start + (1 - block) * run_len, 16), 16)
                mid = hidden_all[block, at].astype(WIDE) + (
                    pair[here].astype(WIDE) + pair_in[there].astype(WIDE)
                )
                mid_out[here] = mid
                scaled = mid * inverse_rms(mid)
                normed[here] = (scaled * gains[1:2]).astype(LOW)

            row_loop(run_len, body)
        give.start()

    greet(fsdp_size)
    line.start()
    start_runs()
    fill_select(select)
    inserts = {
        (2, 1): [tables],
        (2, 2): [first_norm],
        (3, 1): [spread_weights],
        (3, 2): [project_in],
        (3, 3): [lambda: attention(0)],
        (4, 1): [lambda: attention(1)],
        (4, 2): [load_out, project],
        (4, 3): [meet_core],
        (6, 1): [meet_x],
    }
    weave(line.steps(), inserts)
    line.finish(local_done=(0, 1, 2))
    give.wait_recv()
    for copy in (to_core, to_x, give):
        copy.wait_send()
    for bits in (2, 1, 3):
        run_copy(3, bits).wait_recv()
        for r in (0, 1, 2, 3):
            run_copy(r, bits).wait_send()
    run_out().wait()


def gather_front(ctx_size, fsdp_size, collective_id, shards, runs, frequency, heads, kv_heads):
    run_len, width = runs[0].shape
    tokens, half = ctx_size * run_len, 2 * run_len
    few = fsdp_size // ctx_size
    counts = (fsdp_size, fsdp_size, few, fsdp_size, few)
    pieces = (1, 1, 1, 2, 4)
    blocks = []
    for a, shard in enumerate(shards):
        size = shard.shape[0] // pieces[a]
        blocks += [(a, i * size, size) for i in range(pieces[a])]
    fulls = [jax.ShapeDtypeStruct((n, *s.shape), s.dtype) for n, s in zip(counts, shards)]
    columns = shards[1].shape[1]
    padded = (heads + 2 * kv_heads) * 128
    outs = [
        *fulls[1:],
        jax.ShapeDtypeStruct((ctx_size, run_len, width), LOW),
        jax.ShapeDtypeStruct((ctx_size, run_len, width), LOW),
        jax.ShapeDtypeStruct((heads, tokens, 128), LOW),
        jax.ShapeDtypeStruct((kv_heads, tokens, 128), LOW),
        jax.ShapeDtypeStruct((kv_heads, tokens, 128), LOW),
        jax.ShapeDtypeStruct((tokens, tokens), LOW),
        jax.ShapeDtypeStruct((tokens, 128), WIDE),
        jax.ShapeDtypeStruct((tokens, 128), WIDE),
        jax.ShapeDtypeStruct((tokens, width), LOW),
        jax.ShapeDtypeStruct((8, width), WIDE),
        jax.ShapeDtypeStruct((tokens, heads * 128), LOW),
        jax.ShapeDtypeStruct((heads, tokens, 1), WIDE),
        jax.ShapeDtypeStruct((half, width), WIDE),
        jax.ShapeDtypeStruct((tokens, width), LOW),
    ]
    return pl.pallas_call(
        functools.partial(front_kernel, ctx_size, fsdp_size, tuple(blocks), heads, kv_heads),
        out_shape=tuple(outs),
        in_specs=[ANY] * 9 + [VMEM],
        out_specs=(VMEM, ANY, ANY, ANY, VMEM, ANY) + (VMEM,) * 12,
        scratch_shapes=[
            *LineGather.scratch(fsdp_size, shards, len(blocks)),
            pltpu.VMEM(fulls[0].shape, WIDE),
            pltpu.VMEM((ctx_size, *runs[2].shape), WIDE),
            pltpu.VMEM((ctx_size, *runs[3].shape), WIDE),
            pltpu.VMEM((run_len, width), LOW),
            pltpu.VMEM((8, 128), LOW),
            pltpu.VMEM((columns, padded), LOW),
            pltpu.VMEM((width, padded), LOW),
            pltpu.VMEM((heads * 128, width), LOW),
            pltpu.VMEM((half, width), WIDE),
            pltpu.VMEM((half, width), LOW),
            pltpu.VMEM((half, width), LOW),
            pltpu.VMEM((half, width), LOW),
            pltpu.VMEM((half, width), LOW),
            DMA((3,)),
            DMA((3,)),
            DMA((4, 3)),
            DMA((4, 3)),
            DMA((4,)),
            DMA((heads * HEAD_DIM // min(shards[2].shape[0], HEAD_DIM),)),
        ],
        compiler_params=pltpu.CompilerParams(
            collective_id=collective_id, has_side_effects=True, vmem_limit_bytes=58 * 2**20
        ),
    )(*shards, *runs, frequency)


class LineScatter:
    def __init__(self, ctx_size, fsdp_size, kinds, pieces, parts, outs, scratch):
        self.f, self.c, self.z, self.y, self.depth = place(fsdp_size)
        self.n = n = len(parts)
        self.kinds, self.pieces, self.parts, self.outs = kinds, pieces, parts, outs
        self.own, self.beside, self.far = scratch[:n], scratch[n : 2 * n], scratch[2 * n : 3 * n]
        self.cols = [w for w in range(n) if kinds[w] == "cols"]
        count = len(self.cols)
        rest = scratch[3 * n :]
        self.total, self.block, rest = rest[:count], rest[count : 2 * count], rest[2 * count :]
        self.local, self.y_send, self.y_recv, self.z_send, self.z_recv, *more = rest
        if count:
            self.c_send, self.c_recv = more
        self.order = []
        for t in range((self.depth + 1) // 2):
            ends = [self.depth - 1 - t, t]
            self.order += ends if ends[0] != t else [t]
        self.sequence = [(w, t) for w in range(n) for t in self.order]

    @staticmethod
    def shapes(ctx_size, parts, kinds, pieces):
        outs, chunks = [], []
        for part, kind, piece in zip(parts, kinds, pieces):
            if kind == "rows":
                chunks.append(part.shape[1:])
                outs.append(jax.ShapeDtypeStruct(part.shape[1:], WIDE))
                continue
            chunks.append((part.shape[0], *part.shape[2:]))
            rows = part.shape[2]
            for size, flat in piece:
                shape = (rows, ctx_size * size) if flat else (ctx_size, rows, size)
                outs.append(jax.ShapeDtypeStruct(shape, WIDE))
        return outs, chunks

    @staticmethod
    def scratch(fsdp_size, kinds, chunks):
        depth, n = fsdp_size // 2, len(chunks)
        wide = [chunk for chunk, kind in zip(chunks, kinds) if kind == "cols"]
        shapes = [
            *[pltpu.VMEM((depth, *chunk), LOW) for chunk in chunks],
            *[pltpu.VMEM((depth, *chunk), LOW) for chunk in chunks],
            *[pltpu.VMEM((depth + 1, *chunk), LOW) for chunk in chunks],
            *[pltpu.VMEM(chunk, LOW) for chunk in wide],
            *[pltpu.VMEM((3, *chunk[1:]), LOW) for chunk in wide],
            DMA((n, depth)),
            DMA((n, depth)),
            DMA((n, depth)),
            DMA((n, depth)),
            DMA((n, depth + 1)),
        ]
        return shapes + ([DMA((len(wide), 3))] * 2 if wide else [])

    def chunk(self, w, row, column):
        at = row * 2 + column
        return self.parts[w].at[at] if self.kinds[w] == "rows" else self.parts[w].at[:, at]

    def y_copy(self, w, t):
        return remote(
            self.chunk(w, t, 1 - self.y),
            self.beside[w].at[t],
            self.y_send.at[w, t],
            self.y_recv.at[w, t],
            fsdp=self.f ^ 1,
        )

    def z_copy(self, w, t, step, slot):
        return remote(
            self.own[w].at[t],
            self.far[w].at[slot],
            self.z_send.at[w, t],
            self.z_recv.at[w, slot],
            fsdp=(self.z + step) * 2 + self.y,
        )

    def own_copy(self, w, t):
        return pltpu.make_async_copy(self.chunk(w, t, self.y), self.own[w].at[t], self.local.at[w, t])

    def c_copy(self, k, bits):
        return remote(
            self.total[k].at[self.c ^ bits],
            self.block[k].at[bits - 1],
            self.c_send.at[k, bits - 1],
            self.c_recv.at[k, bits - 1],
            ctx=self.c ^ bits,
        )

    def start(self, ready):
        for w, t in self.sequence[:AHEAD]:
            self.y_copy(w, t).start()
        self.load(range(ready))

    def load(self, groups):
        for w in groups:
            for t in self.order:
                self.own_copy(w, t).start()

    def send_on(self, w, t, step, ahead):
        slot = t if step == 1 else t + jnp.where(ahead == 1, self.depth - t, 0)
        self.z_copy(w, t, step, slot).start()

    def near(self, index):
        w, t = self.sequence[index]
        own = self.own[w].at[t]
        self.own_copy(w, t).wait()
        self.y_copy(w, t).wait_recv()
        if index + AHEAD < len(self.sequence):
            self.y_copy(*self.sequence[index + AHEAD]).start()
        for step in (1, -1):
            ahead = (t - self.z) * step
            last = self.z == (0 if step == 1 else self.depth - 1)

            @pl.when((ahead > 0) & last)
            def _():
                add_rows(own, (own, self.beside[w].at[t]))
                self.send_on(w, t, step, ahead)

    def relay(self, index):
        w, t = self.sequence[index]
        own = self.own[w].at[t]
        for step in (1, -1):
            ahead = (t - self.z) * step
            behind = (self.z - step >= 0) & (self.z - step < self.depth)

            @pl.when((ahead > 0) & behind)
            def _():
                self.z_copy(w, t, step, t).wait_recv()
                add_rows(own, (own, self.beside[w].at[t], self.far[w].at[t]))
                self.send_on(w, t, step, ahead)

    def first_out(self, w):
        return sum(
            1 if self.kinds[v] == "rows" else len(self.pieces[v]) for v in range(w)
        )

    def settle(self, w):
        z, depth = self.z, self.depth
        pl.when(z > 0)(lambda: self.z_copy(w, 0, 1, z).wait_recv())
        pl.when(z < depth - 1)(lambda: self.z_copy(w, 0, 1, depth).wait_recv())
        rows = self.kinds[w] == "rows"
        target = self.outs[self.first_out(w)] if rows else self.total[self.cols.index(w)]
        home = [self.own[w].at[z], self.beside[w].at[z]]
        below, above = self.far[w].at[z], self.far[w].at[depth]
        pl.when(z == 0)(lambda: add_rows(target, (*home, above)))
        pl.when(z == depth - 1)(lambda: add_rows(target, (*home, below)))
        pl.when((z > 0) & (z < depth - 1))(lambda: add_rows(target, (*home, below, above)))
        if not rows:
            for bits in (1, 2, 3):
                self.c_copy(self.cols.index(w), bits).start()

    def spread(self, w):
        k, first = self.cols.index(w), self.first_out(w)
        for bits in (0, 1, 2, 3):
            if bits:
                self.c_copy(k, bits).wait_recv()
            source = self.total[k].at[self.c] if bits == 0 else self.block[k].at[bits - 1]
            at = 0
            for j, (size, flat) in enumerate(self.pieces[w]):
                value = source[:, at : at + size].astype(WIDE)
                if flat:
                    where = pl.ds(pl.multiple_of((self.c ^ bits) * size, 128), size)
                    self.outs[first + j][:, where] = value
                else:
                    self.outs[first + j][self.c ^ bits] = value
                at += size

    def steps(self):
        result = []
        count = len(self.sequence)
        for k in range(count + 1):
            if k < count:
                result.append((("near", k), functools.partial(self.near, k)))
            if k:
                result.append((("relay", k - 1), functools.partial(self.relay, k - 1)))
            w = k // self.depth - 1
            if k % self.depth == 0 and w >= 1:
                result.append((("settle", w - 1), functools.partial(self.settle, w - 1)))
                if w - 2 in self.cols:
                    result.append((("spread", w - 2), functools.partial(self.spread, w - 2)))
        result.append((("settle", self.n - 1), functools.partial(self.settle, self.n - 1)))
        for w in self.cols:
            if w >= self.n - 2:
                result.append((("spread", w), functools.partial(self.spread, w)))
        return result

    def finish(self):
        for w, t in self.sequence:
            self.y_copy(w, t).wait_send()
            for step in (1, -1):
                pl.when((t - self.z) * step > 0)(
                    lambda w=w, t=t, step=step: self.z_copy(w, t, step, t).wait_send()
                )
        for k in range(len(self.cols)):
            for bits in (1, 2, 3):
                self.c_copy(k, bits).wait_send()


def back_kernel(ctx_size, fsdp_size, kinds, pieces, n_out, heads, kv_heads, *refs):
    n_in = len(kinds) - 2
    parts, refs = refs[:n_in], refs[n_in:]
    far_half, out_far, w_full, w_qkv, near_half, out_near, mid, cot, refs = *refs[:8], refs[8:]
    gains, query, key, value, bias, log, rows, refs = *refs[:7], refs[7:]
    cosine, sine, normed, hidden, refs = *refs[:4], refs[4:]
    outs, refs = refs[:n_out], refs[n_out:]
    output, grad_in, gain_out, refs = *refs[:3], refs[3:]
    part_qkv, part_out, w_pad, w_proj, select, core_in, pair, pair_in, refs = *refs[:8], refs[8:]
    grad_ffn, grad_mid, mid_low, grad_rows, refs = *refs[:4], refs[4:]
    grad_key, grad_value, grad_pad, grad_low, in_near, in_far, refs = *refs[:6], refs[6:]
    last_in, swap_out, swap_in, gain_own, gain_in, gain_far, refs = *refs[:6], refs[6:]
    c_send, c_recv, g_send, g_recv, w_sem, *scratch = refs
    f, c, z, y, depth = place(fsdp_size)
    line = LineScatter(
        ctx_size, fsdp_size, kinds, pieces, (*parts, part_qkv, part_out), outs, scratch
    )
    tokens, half = query.shape[1], mid.shape[0]
    run_len, tile = half // 2, 128
    owned = part_qkv.shape[2]
    scale = HEAD_DIM**-0.5

    def exchange(index, src, dst, bits):
        return remote(src, dst, c_send.at[index], c_recv.at[index], ctx=c ^ bits)

    to_core = exchange(0, far_half, core_in, 1)
    to_x = exchange(1, pair, pair_in, 2)
    give = exchange(2, mid_low.at[pl.ds(0, half)], mid_low.at[pl.ds(half, half)], 1)
    cores = [exchange(3, in_far, last_in.at[0], 1), exchange(4, out_far, last_in.at[1], 1)]
    swaps = [exchange(5 + i, swap_out.at[i], swap_in.at[i], 2) for i in (0, 1)]
    shard = w_full.shape[1]
    piece = min(shard, HEAD_DIM)
    moves = []
    for at in range(0, heads * HEAD_DIM, piece):
        to = at // HEAD_DIM * 128 + at % HEAD_DIM
        src = w_full.at[at // shard, pl.ds(at % shard, piece)]
        moves.append(pltpu.make_async_copy(src, w_pad.at[pl.ds(to, piece)], w_sem.at[len(moves)]))
    move_proj = pltpu.make_async_copy(w_qkv, w_proj, w_sem.at[len(moves)])

    def load_weights():
        for move in moves:
            move.start()
        move_proj.start()
        for h in range(heads):
            w_pad[pl.ds(h * 128 + HEAD_DIM, 128 - HEAD_DIM)] = jnp.zeros(
                (128 - HEAD_DIM, w_pad.shape[1]), LOW
            )
        fill_select(select)

    def meet_core():
        to_core.wait_recv()
        add_rows(pair, (near_half, core_in))
        to_x.start()

    def meet_x():
        to_x.wait_recv()
        for block in (0, 1):

            def body(at, block=block):
                here = pl.ds(pl.multiple_of(at.start + block * run_len, 16), 16)
                there = pl.ds(pl.multiple_of(at.start + (1 - block) * run_len, 16), 16)
                grad = pair[here].astype(WIDE) + pair_in[there].astype(WIDE)
                grad_ffn[here] = grad
                recip = inverse_rms(mid[here])
                scaled = mid[here] * recip
                total = cot[here].astype(WIDE) + norm_backward(grad, scaled, recip, gains[1:2])
                grad_mid[here] = total
                mid_low[here] = total.astype(LOW)

            row_loop(run_len, body)
        give.start()
        for move in moves:
            move.wait()
        move_proj.wait()

    def attend_back():
        give.wait_recv()

        def back_out(at):
            grad_rows[at] = lax.dot_general(
                mid_low[at], w_pad[...], (((1,), (1,)), ((), ())), preferred_element_type=WIDE
            ).astype(LOW)

        row_loop(tokens, back_out, tile)
        grad_key[...] = jnp.zeros_like(grad_key)
        grad_value[...] = jnp.zeros_like(grad_value)

        def body(i, carry):
            h = i // (tokens // tile)
            r = i % (tokens // tile)
            at = pl.ds(pl.multiple_of(r * tile, tile), tile)
            lanes = pl.ds(pl.multiple_of(h * 128, 128), 128)
            g = h // (heads // kv_heads)
            q = query[h, at]
            s = lax.dot_general(
                q, key[g], (((1,), (1,)), ((), ())), preferred_element_type=WIDE
            )
            p = jnp.exp(s * scale + bias[at].astype(WIDE) - log[h, at])
            grad_out = grad_rows[at, lanes]
            delta = jnp.sum(
                grad_out.astype(WIDE) * rows[at, lanes].astype(WIDE), axis=-1, keepdims=True
            )
            grad_p = lax.dot_general(
                grad_out, value[g], (((1,), (1,)), ((), ())), preferred_element_type=WIDE
            )
            grad_s = (p * (grad_p - delta)).astype(LOW)
            turned = jnp.dot(grad_s, key[g], preferred_element_type=WIDE) * scale
            grad_pad[at, lanes] = turn(turned, cosine[at], -sine[at]).astype(LOW)
            grad_key[g] = grad_key[g] + contract_rows(grad_s, q)
            grad_value[g] = grad_value[g] + contract_rows(p.astype(LOW), grad_out)
            return carry

        lax.fori_loop(0, heads * (tokens // tile), body, 0)
        for g in range(kv_heads):
            for r in range(tokens // tile):
                at = pl.ds(r * tile, tile)
                turned = turn(grad_key[g, at] * scale, cosine[at], -sine[at])
                grad_pad[at, pl.ds((heads + g) * 128, 128)] = turned.astype(LOW)
                grad_pad[at, pl.ds((heads + kv_heads + g) * 128, 128)] = grad_value[g, at].astype(
                    LOW
                )

    def project_back():
        def compact(at):
            grad_low[at] = lax.dot_general(
                grad_pad[at], select[...], (((1,), (1,)), ((), ())), preferred_element_type=WIDE
            ).astype(LOW)

        row_loop(tokens, compact, tile)

        def far(at):
            there = pl.ds(pl.multiple_of(at.start + half, tile), tile)
            in_far[at] = times_transpose(grad_low[there], w_proj[...]).astype(LOW)

        row_loop(half, far, tile)
        cores[0].start()

        def near(at):
            in_near[at] = times_transpose(grad_low[at], w_proj[...])

        row_loop(half, near, tile)

    def weight_grads():
        count = w_proj.shape[0] // ctx_size
        for q in range(ctx_size):
            grads = contract_rows(normed[:, q * count : (q + 1) * count], grad_low[...]).astype(LOW)
            for e in range(fsdp_size):
                part_qkv[q, e] = grads[e * owned : (e + 1) * owned]
        for h in range(heads):
            grads = contract_rows(rows[:, h * 128 : (h + 1) * 128], mid_low[...]).astype(LOW)
            for e in range(HEAD_DIM // owned):
                part_out[h * (HEAD_DIM // owned) + e] = grads[e * owned : (e + 1) * owned]
        line.load((n_in, n_in + 1))

    near = (in_near, out_near)

    def last_core(i):
        cores[i].wait_recv()

        def body(at):
            there = pl.ds(pl.multiple_of(at.start + run_len, 16), 16)
            swap_out[i, at] = (near[i][there].astype(WIDE) + last_in[i, there].astype(WIDE)).astype(LOW)

        row_loop(run_len, body)
        swaps[i].start()

    def own_sum(i, at):
        mine = near[i][at].astype(WIDE) + last_in[i, at].astype(WIDE)
        return mine + swap_in[i, at].astype(WIDE)

    def last_in_sum():
        swaps[0].wait_recv()
        gain_own[...] = jnp.zeros_like(gain_own)

        def body(at):
            grad = own_sum(0, at)
            values = hidden[at].astype(WIDE)
            recip = inverse_rms(values)
            scaled = values * recip
            grad_in[at] = grad_mid[at] + norm_backward(grad, scaled, recip, gains[0:1])
            gain_own[0, 0:1] = gain_own[0, 0:1] + jnp.sum(grad * scaled, axis=0, keepdims=True)
            mids = mid[at]
            gain_own[0, 1:2] = gain_own[0, 1:2] + jnp.sum(
                grad_ffn[at] * (mids * inverse_rms(mids)), axis=0, keepdims=True
            )

        row_loop(run_len, body)

    def last_out_sum():
        swaps[1].wait_recv()

        def body(at):
            output[at] = (mid[at] + own_sum(1, at)).astype(LOW)

        row_loop(run_len, body)

    def gain_copy(i):
        where = ({"ctx": c ^ 1}, {"ctx": c ^ 2}, {"fsdp": f ^ 1})[i]
        return remote(gain_own.at[i], gain_in.at[i], g_send.at[i], g_recv.at[i], **where)

    def gain_row(shift):
        return remote(
            gain_own.at[3],
            gain_far.at[shift - 1],
            g_send.at[2 + shift],
            g_recv.at[2 + shift],
            fsdp=(z + shift) % depth * 2 + y,
        )

    def gain_meet(i):
        if i:
            gain_copy(i - 1).wait_recv()
            gain_own[i] = gain_own[i - 1] + gain_in[i - 1]
        if i < 3:
            gain_copy(i).start()
            return
        for shift in range(1, depth):
            gain_row(shift).start()

    def gain_end():
        total = gain_own[3]
        for shift in range(1, depth):
            gain_row(shift).wait_recv()
            total = total + gain_far[shift - 1]
        gain_out[...] = total

    greet(fsdp_size, all_rows=True)
    to_core.start()
    cores[1].start()
    line.start(n_in)
    inserts = {
        ("near", 0): [load_weights, meet_core, meet_x],
        ("near", 1): [attend_back],
        ("relay", 0): [project_back],
        ("near", 2): [lambda: last_core(0)],
        ("near", 3): [weight_grads, lambda: last_core(1)],
        ("near", 5): [last_in_sum, lambda: gain_meet(0)],
        ("near", 6): [lambda: gain_meet(1), last_out_sum],
        ("near", 7): [lambda: gain_meet(2)],
        ("near", 9): [lambda: gain_meet(3)],
    }
    weave(line.steps(), inserts)
    gain_end()
    line.finish()
    for copy in (to_core, to_x, give, *cores, *swaps, *[gain_copy(i) for i in range(3)]):
        copy.wait_send()
    for shift in range(1, depth):
        gain_row(shift).wait_send()


def turn(tensor, cosine, sine):
    lane = lax.broadcasted_iota(jnp.int32, tensor.shape, 1)
    half_dim = HEAD_DIM // 2
    moved = jnp.where(
        lane < half_dim,
        -pltpu.roll(tensor, 128 - half_dim, 1),
        pltpu.roll(tensor, half_dim, 1),
    )
    return tensor * cosine + moved * sine


def fill_select(select):
    def body(at):
        shape = (at.size, select.shape[1])
        row = lax.broadcasted_iota(jnp.int32, shape, 0) + at.start
        lane = lax.broadcasted_iota(jnp.int32, shape, 1)
        inner = lane & 127
        column = (lane >> 7) * HEAD_DIM + inner
        select[at] = jnp.where((row == column) & (inner < HEAD_DIM), 1.0, 0.0).astype(LOW)

    row_loop(select.shape[0], body, 128)


def scatter_back(ctx_size, fsdp_size, collective_id, parts, kinds, pieces, small):
    far_half, out_far, w_full, w_qkv, near_half, out_near, mid, cot = small[:8]
    gains, query, key = small[8:11]
    half, width = mid.shape
    heads, tokens, _ = query.shape
    kv_heads = key.shape[0]
    owned = width // (ctx_size * fsdp_size)
    columns = w_qkv.shape[1]
    part_qkv = jax.ShapeDtypeStruct((ctx_size, fsdp_size, owned, columns), LOW)
    part_out = jax.ShapeDtypeStruct((fsdp_size, owned, width), LOW)
    outs, chunks = LineScatter.shapes(ctx_size, (*parts, part_qkv, part_out), kinds, pieces)
    n_out = len(outs)
    run_len = half // 2
    outs += [
        jax.ShapeDtypeStruct((run_len, width), LOW),
        jax.ShapeDtypeStruct((run_len, width), WIDE),
        jax.ShapeDtypeStruct((8, width), WIDE),
    ]
    depth = fsdp_size // 2
    padded = (heads + 2 * kv_heads) * 128
    results = pl.pallas_call(
        functools.partial(back_kernel, ctx_size, fsdp_size, kinds, pieces, n_out, heads, kv_heads),
        out_shape=tuple(outs),
        in_specs=[ANY] * (len(parts) + 4) + [VMEM] * (len(small) - 4),
        out_specs=(VMEM,) * len(outs),
        scratch_shapes=[
            pltpu.VMEM(part_qkv.shape, LOW),
            pltpu.VMEM(part_out.shape, LOW),
            pltpu.VMEM((heads * 128, width), LOW),
            pltpu.VMEM(w_qkv.shape, LOW),
            pltpu.VMEM((columns, padded), LOW),
            pltpu.VMEM((half, width), LOW),
            pltpu.VMEM((half, width), LOW),
            pltpu.VMEM((half, width), LOW),
            pltpu.VMEM((half, width), WIDE),
            pltpu.VMEM((half, width), WIDE),
            pltpu.VMEM((tokens, width), LOW),
            pltpu.VMEM((tokens, heads * 128), LOW),
            pltpu.VMEM(key.shape, WIDE),
            pltpu.VMEM(key.shape, WIDE),
            pltpu.VMEM((tokens, padded), LOW),
            pltpu.VMEM((tokens, columns), LOW),
            pltpu.VMEM((half, width), WIDE),
            pltpu.VMEM((half, width), LOW),
            pltpu.VMEM((2, half, width), LOW),
            pltpu.VMEM((2, run_len, width), LOW),
            pltpu.VMEM((2, run_len, width), LOW),
            pltpu.VMEM((4, 8, width), WIDE),
            pltpu.VMEM((3, 8, width), WIDE),
            pltpu.VMEM((depth - 1, 8, width), WIDE),
            DMA((7,)),
            DMA((7,)),
            DMA((2 + depth,)),
            DMA((2 + depth,)),
            DMA((heads * HEAD_DIM // min(w_full.shape[1], HEAD_DIM) + 1,)),
            *LineScatter.scratch(fsdp_size, kinds, chunks),
        ],
        compiler_params=pltpu.CompilerParams(
            collective_id=collective_id, has_side_effects=True, vmem_limit_bytes=63 * 2**20
        ),
    )(*parts, *small)
    return results[:n_out], results[n_out:]


def inverse_rms(values):
    return lax.rsqrt(jnp.mean(values * values, axis=-1, keepdims=True) + EPS)


def norm_backward(grad_normed, scaled, inv_rms, gain):
    grad_scaled = grad_normed * gain
    return inv_rms * (
        grad_scaled - scaled * jnp.mean(grad_scaled * scaled, axis=-1, keepdims=True)
    )


def dot(left, right):
    return jnp.dot(left, right, preferred_element_type=jnp.float32)


def contract_rows(left, right):
    return lax.dot_general(
        left, right, (((0,), (0,)), ((), ())), preferred_element_type=jnp.float32
    )


def times_transpose(left, weight):
    return lax.dot_general(
        left, weight, (((1,), (1,)), ((), ())), preferred_element_type=jnp.float32
    )


def make_step(ctx_size, fsdp_size):
    def per_device(
        hidden_in,
        segments,
        w_query,
        w_key,
        w_value,
        w_out,
        w_gate,
        w_up,
        w_down,
        attn_gain,
        ffn_gain,
        grad_out,
    ):
        _, run_len, width = hidden_in.shape
        c_index, f_index = lax.axis_index("ctx"), lax.axis_index("fsdp")
        heads, kv_heads = HEADS // ctx_size, KV_HEADS // ctx_size
        q_cols, kv_cols = heads * HEAD_DIM, kv_heads * HEAD_DIM
        ff = w_gate.shape[1] // ctx_size
        shard = width // fsdp_size
        owned = shard // ctx_size
        half = 2 * run_len

        def columns(weight, size):
            return lax.dynamic_slice_in_dim(weight, c_index * size, size, 1)

        own_hidden = hidden_in.reshape(run_len, width)
        own_seg = segments.astype(WIDE)
        half_dim = HEAD_DIM // 2
        freq_index = jnp.arange(half_dim, dtype=WIDE)
        frequency = jnp.exp(freq_index * (-2.0 / HEAD_DIM) * math.log(ROPE_BASE))
        frequency = jnp.pad(jnp.concatenate([frequency, frequency]), (0, 128 - HEAD_DIM))
        (
            full_qkv,
            full_out,
            full_gate_up,
            full_down,
            _,
            cotangent,
            query,
            key,
            value,
            bias,
            cosine,
            sine,
            attn_normed,
            gains,
            attn_rows,
            log_total,
            mid,
            ffn_normed,
        ) = gather_front(
            ctx_size,
            fsdp_size,
            0,
            (
                jnp.pad(
                    jnp.stack([attn_gain, ffn_gain]).astype(WIDE), ((0, 6), (0, -shard % 128))
                ),
                jnp.concatenate(
                    [columns(w_query, q_cols), columns(w_key, kv_cols), columns(w_value, kv_cols)],
                    axis=1,
                ),
                w_out,
                jnp.concatenate([columns(w_gate, ff), columns(w_up, ff)], axis=1),
                w_down,
            ),
            (
                own_hidden,
                grad_out.reshape(run_len, width),
                jnp.broadcast_to(own_seg, (8, run_len)),
                jnp.broadcast_to(own_seg.T, (run_len, 128)),
            ),
            jnp.broadcast_to(frequency, (8, 128)),
            heads,
            kv_heads,
        )
        full_qkv = full_qkv.reshape(width, q_cols + 2 * kv_cols)
        full_gate_up = full_gate_up.reshape(width, 2 * ff)
        full_down = full_down.reshape(ff, width)
        cotangent = cotangent.reshape(-1, width)

        gate_up = dot(ffn_normed, full_gate_up)
        gate, up = gate_up[:, :ff], gate_up[:, ff:]
        sigmoid = jax.nn.sigmoid(gate)
        silu = gate * sigmoid
        inner = (silu * up).astype(LOW)
        part_output = dot(inner, full_down)
        part_down = contract_rows(inner, cotangent).astype(LOW)
        grad_inner = times_transpose(cotangent, full_down)
        grad_gate = grad_inner * up * sigmoid * (1.0 + gate * (1.0 - sigmoid))
        grad_gate_up = jnp.concatenate(
            [grad_gate.astype(LOW), (grad_inner * silu).astype(LOW)], axis=1
        )
        part_ffn = times_transpose(grad_gate_up, full_gate_up)
        part_gate_up = contract_rows(ffn_normed, grad_gate_up).astype(LOW)

        grads, (output, grad_in, gain_sums) = scatter_back(
            ctx_size,
            fsdp_size,
            1,
            (
                part_gate_up.reshape(ctx_size, fsdp_size, owned, 2 * ff),
                part_down.reshape(fsdp_size, -1, width),
            ),
            ("cols", "rows", "cols", "rows"),
            (((ff, True), (ff, True)), None, ((q_cols, True), (2 * kv_cols, False)), None),
            (
                part_ffn[half:].astype(LOW),
                part_output[half:].astype(LOW),
                full_out,
                full_qkv,
                part_ffn[:half],
                part_output[:half].astype(LOW),
                mid,
                cotangent[:half],
                gains,
                query,
                key,
                value,
                bias,
                log_total,
                attn_rows,
                cosine,
                sine,
                attn_normed,
                own_hidden,
            ),
        )
        grad_gate_w, grad_up_w, grad_down_w, grad_query_w, grad_kv_w, grad_out_w = grads
        grad_kv_w = jnp.swapaxes(grad_kv_w, 0, 1)
        gain_own = lax.dynamic_slice_in_dim(
            gain_sums[:2], (c_index * fsdp_size + f_index) * owned, owned, 1
        )

        return (
            output[None],
            grad_in[None],
            grad_query_w,
            grad_kv_w[:, :, :kv_cols].reshape(owned, -1),
            grad_kv_w[:, :, kv_cols:].reshape(owned, -1),
            grad_out_w,
            grad_gate_w,
            grad_up_w,
            grad_down_w,
            gain_own[0],
            gain_own[1],
        )

    return per_device


def solution(mesh):
    rows = P("fsdp", None)
    spread = P(("ctx", "fsdp"), None)
    runs = P("fsdp", "ctx", None)
    return jax.shard_map(
        make_step(mesh.shape["ctx"], mesh.shape["fsdp"]),
        mesh=mesh,
        in_specs=(runs, P("fsdp", "ctx"), *[rows] * 7, P("fsdp"), P("fsdp"), runs),
        out_specs=(runs, runs, *[spread] * 7, P(("ctx", "fsdp")), P(("ctx", "fsdp"))),
        check_vma=False,
    )
```
